256 devices in a mesh: mode: 64 (over y, z, core), row: 4 (over x).
Axes of the slice: x: 4, y: 4, z: 8, core: 2. Of those that a mesh axis runs over, the one named last changes fastest.
Arguments:
- density: float32 [2, 2048, 2048], P(None, 'row', 'mode'), may hold values from -6 to 6
- auxiliary: float32 [2048, 256, 2, 128], P('row', 'mode'), may hold values from -2 to 2
- hamiltonian: bfloat16 [2048, 2048], P('row'), as said below
- coupling: int32 [2, 128], replicated, may hold values from 0 to 2047, as said below
- lead_index: int32 [256], P('mode'), may hold values from 0 to 1
- mode_level: float32 [256], P('mode'), may hold values from -2 to 2
- mode_width: float32 [256], P('mode'), may hold values from 0.05 to 3
- residue: float32 [256, 2], P('mode'), may hold values from -4 to 4
- occupation: float32 [256], P('mode'), may hold values from 0 to 1
- lead_gamma: bfloat16 [2, 128, 128], replicated, may hold values from -0.5 to 0.5
Outputs:
- density_rate: float32 [2, 2048, 2048], P(None, 'row', 'mode')
- auxiliary_rate: float32 [2048, 256, 2, 128], P('row', 'mode')
The draws below stay inside these ranges and needn't reach their ends.
Inputs may be any that keep to these rules, and one draw needn't show every extreme that they name: `coupling`: all 256 entries are distinct orbitals. `hamiltonian`: Symmetric.
All inputs are finite; a program needn't handle non-finite values.
Results may differ from the reference program's by a relative error of at most 0.0044.
Values may be sent and summed in bfloat16 or wider, within the bound.
A program may use at most 128 MiB of HBM per device.

```python
import math
import jax
import jax.numpy as jnp
from jax import lax

N = 2048
NC = 128
LEADS = 2
MODE_DEV = 4
MODES = 256
N_MODE = 64


def draw_hamiltonian(key, part):
    values = jax.random.normal(key, (N, N), jnp.float32)
    symmetric = (values + values.T) * 0.5 ** 0.5 / math.sqrt(N)
    return symmetric.astype(jnp.bfloat16)


def draw_coupling(key, part):
    ordering = jax.random.permutation(jax.random.fold_in(key, 7), N)
    return ordering[:LEADS * NC].reshape(LEADS, NC).astype(jnp.int32)


def plant(drawn, stream_key, low, largest):
    dims = drawn.shape
    index_at = [jax.random.randint(jax.random.fold_in(stream_key, axis), (), 0, dims[axis]) for axis in range(len(dims))]
    drawn = drawn.at[tuple(index_at)].set(low)
    longest = dims.index(max(dims))
    index_at[longest] = (index_at[longest] + 1) % dims[longest]
    return drawn.at[tuple(index_at)].set(largest)


def shard_levels(stream_key, dims, split, low, largest):
    def one(position, parts):
        steps = jax.random.uniform(jax.random.fold_in(jax.random.fold_in(stream_key, 6), position), (parts,), jnp.float32, low / len(split), largest / len(split))
        return jnp.repeat(jnp.exp(steps), dims[position] // parts).reshape((-1,) + (1,) * (len(dims) - position - 1))

    factor_of = one(*split[0])
    for cut in split[1:]:
        factor_of = factor_of * one(*cut)
    return factor_of


def bell_draw(rng, shape, spread, limit, shards=(), held_as=jnp.bfloat16):
    level = shard_levels(rng, shape, shards, -0.22, 0.18) if shards else 1.0
    drawn = jax.random.normal(rng, shape, jnp.float32) * spread * level
    return jnp.minimum(jnp.maximum(drawn, -limit), limit).astype(held_as)


def setup_inputs(seed: int = 0) -> dict:
    key_of = jax.random.split(jax.random.key(seed), 11)
    return {
        "density": bell_draw(key_of[0], (2, N, N), 1.0, 6.0, ((1, 4), (2, 64)), jnp.float32),
        "auxiliary": bell_draw(key_of[1], (N, MODES, 2, NC), 0.3, 2.0, ((0, 4), (1, 64)), jnp.float32),
        "hamiltonian": draw_hamiltonian(jax.random.fold_in(key_of[10], 71), 0),
        "coupling": draw_coupling(jax.random.fold_in(key_of[10], 71), 0),
        "lead_index": plant(jax.random.randint(key_of[4], (MODES,), 0, LEADS), jax.random.fold_in(key_of[4], 1), 0, LEADS - 1).astype(jnp.int32),
        "mode_level": jnp.clip(jax.random.uniform(key_of[5], (MODES,), jnp.float32, -2.0, 2.0) * shard_levels(key_of[5], (MODES,), ((0, 64),), -0.4, 0.0), -2.0, 2.0),
        "mode_width": jnp.clip(jnp.exp(math.log(3.0) - 4.0943445 * jax.random.uniform(key_of[6], (MODES,), jnp.float32) ** shard_levels(key_of[6], (MODES,), ((0, 64),), -0.2, 0.2)), 0.05, 3.0),
        "residue": bell_draw(key_of[7], (MODES, 2), 1.0, 4.0, ((0, 64),), jnp.float32),
        "occupation": jnp.clip(1.0 * jax.random.uniform(key_of[8], (MODES,), jnp.float32) ** shard_levels(key_of[8], (MODES,), ((0, 64),), -0.2, 0.2), 0.0, 1.0),
        "lead_gamma": bell_draw(key_of[9], (LEADS, NC, NC), NC ** -0.5, 0.5),
    }


step_size = 0.1
highest = lax.Precision.HIGHEST


def rho_rates(state, hamiltonian, lead_sums, select):
    dens_b = state.astype(jnp.bfloat16)
    ham_rho = jnp.stack([jnp.dot(hamiltonian, dens_b[component], preferred_element_type=jnp.float32) for component in range(2)])
    rho_ham = jnp.stack([jnp.dot(dens_b[component], hamiltonian, preferred_element_type=jnp.float32) for component in range(2)])
    forward = jnp.stack([jnp.dot(lead_sums[:, component, :], select.T, precision=highest) for component in range(2)])
    commutator = ham_rho - rho_ham
    real_part = commutator[1] + forward[0] + forward[0].T
    imag_part = -commutator[0] + forward[1] - forward[1].T
    return jnp.stack([real_part, imag_part])


def source_terms(state, lead_gamma, flat_coupling):
    dens_b = state.astype(jnp.bfloat16)
    coupled_rho = jnp.take(dens_b, flat_coupling, axis=2).astype(jnp.float32).reshape(2, N, LEADS, NC)
    return jnp.einsum("cali,lij->calj", coupled_rho, lead_gamma.astype(jnp.float32))


def aux_rates(state_aux, hamiltonian, sources, gamma_rows, onehot, level, width, residue, occupation):
    ham_aux = jnp.dot(hamiltonian, state_aux.astype(jnp.bfloat16).reshape(N, -1), preferred_element_type=jnp.float32).reshape(state_aux.shape)
    picked = jnp.einsum("calj,kl->akcj", sources, onehot, precision=highest)
    picked_rows = jnp.einsum("alj,kl->akj", gamma_rows, onehot, precision=highest)
    driven = picked - occupation[None, :, None, None] * picked_rows[:, :, None, :]
    shifted = ham_aux - level[None, :, None, None] * state_aux
    decay = width[None, :, None]
    res_re = residue[:, 0][None, :, None]
    res_im = residue[:, 1][None, :, None]
    aux_re = shifted[:, :, 1, :] - decay * state_aux[:, :, 0, :] + res_re * driven[:, :, 0, :] - res_im * driven[:, :, 1, :]
    aux_im = -shifted[:, :, 0, :] - decay * state_aux[:, :, 1, :] + res_re * driven[:, :, 1, :] + res_im * driven[:, :, 0, :]
    return jnp.stack([aux_re, aux_im], axis=2)


def reference(density, auxiliary, hamiltonian, coupling, lead_index, mode_level, mode_width, residue, occupation, lead_gamma):
    flat_coupling = coupling.reshape(-1).astype(jnp.int32)
    select = (jnp.arange(N, dtype=jnp.int32)[:, None] == flat_coupling[None, :]).astype(jnp.float32)
    onehot = (lead_index[:, None] == jnp.arange(LEADS, dtype=jnp.int32)[None, :]).astype(jnp.float32)
    sums_first = jnp.einsum("akcj,kl->aclj", auxiliary, onehot, precision=highest).reshape(N, 2, LEADS * NC)
    first_rho = rho_rates(density, hamiltonian, sums_first, select)
    middle = density + 0.5 * step_size * first_rho
    src_first = source_terms(density, lead_gamma, flat_coupling)
    src_second = source_terms(middle, lead_gamma, flat_coupling)
    gamma_rows = jnp.einsum("alj,ljk->alk", select.reshape(N, LEADS, NC), lead_gamma.astype(jnp.float32), precision=highest)
    aux_blocks = auxiliary.reshape(N, N_MODE, MODE_DEV, 2, NC).transpose(1, 0, 2, 3, 4)

    def advance(total, inputs):
        aux_blk, hot_blk, lev_blk, wid_blk, res_blk, occ_blk = inputs
        first = aux_rates(aux_blk, hamiltonian, src_first, gamma_rows, hot_blk, lev_blk, wid_blk, res_blk, occ_blk)
        moved = aux_blk + 0.5 * step_size * first
        second = aux_rates(moved, hamiltonian, src_second, gamma_rows, hot_blk, lev_blk, wid_blk, res_blk, occ_blk)
        total = total + jnp.einsum("akcj,kl->aclj", moved, hot_blk, precision=highest).reshape(N, 2, LEADS * NC)
        return total, first + 2.0 * second

    inputs = (aux_blocks, onehot.reshape(N_MODE, MODE_DEV, LEADS), mode_level.reshape(N_MODE, MODE_DEV),
              mode_width.reshape(N_MODE, MODE_DEV), residue.reshape(N_MODE, MODE_DEV, 2), occupation.reshape(N_MODE, MODE_DEV))
    sums_second, blocks_out = lax.scan(advance, jnp.zeros((N, 2, LEADS * NC), jnp.float32), inputs)
    auxiliary_rate = blocks_out.transpose(1, 0, 2, 3, 4).reshape(N, N_MODE * MODE_DEV, 2, NC)
    second_rho = rho_rates(middle, hamiltonian, sums_second, select)
    return first_rho + 2.0 * second_rho, auxiliary_rate
```

```python
import jax
import jax.numpy as jnp
from jax import lax
from jax.sharding import PartitionSpec as P

H2 = 0.05
F32 = jnp.float32
BF = jnp.bfloat16


def dot(a, b, ca=1, cb=0):
    return lax.dot_general(a, b, (((ca,), (cb,)), ((), ())), preferred_element_type=F32)


def over_row(x):
    devices = lax.axis_size("row")
    return lax.all_to_all(jnp.broadcast_to(x[None], (devices, *x.shape)), "row", 0, 0, tiled=True)


def by_lead(x, gamma):
    leads, coupled = gamma.shape[:2]
    return jnp.concatenate(
        [dot(x[:, l * coupled : (l + 1) * coupled], gamma[l]) for l in range(leads)], axis=1
    )


def shards(density, auxiliary, hamiltonian, coupling, lead_index, mode_level, mode_width, residue, occupation, lead_gamma):
    rows, cols = density.shape[1:]
    n = hamiltonian.shape[1]
    leads, coupled = coupling.shape
    q = leads * coupled
    modes = auxiliary.shape[1]
    n_mode = lax.axis_size("mode")
    n_row = lax.axis_size("row")
    x_pos, m_pos = lax.axis_index("row"), lax.axis_index("mode")
    row_start, col_start = x_pos * rows, m_pos * cols
    flat = coupling.reshape(-1)

    e_full = (jnp.arange(n, dtype=jnp.int32)[:, None] == flat[None, :]).astype(BF)
    e_row = (row_start + jnp.arange(rows, dtype=jnp.int32)[:, None] == flat[None, :]).astype(BF)
    e_col = (col_start + jnp.arange(cols, dtype=jnp.int32)[:, None] == flat[None, :]).astype(BF)
    g_row = by_lead(e_row, lead_gamma).astype(BF)
    g_col = by_lead(e_col, lead_gamma).astype(BF)

    rho_t = jnp.swapaxes(density, 1, 2).astype(BF).reshape(2 * cols, rows)
    ham_ct = jnp.swapaxes(lax.dynamic_slice_in_dim(hamiltonian, col_start, cols, 1), 0, 1)

    first = over_row(jnp.concatenate([ham_ct, rho_t], axis=0))
    first = jnp.moveaxis(first, 0, 1).reshape(3 * cols, n)
    ham_c = first[:cols]
    applied = dot(first, hamiltonian, 1, 1)
    ham2_ct = applied[:cols].astype(BF)
    hrho_t = applied[cols:]
    he_row = dot(hamiltonian, e_full)
    hg_row = by_lead(he_row.astype(BF), lead_gamma)
    he_col = dot(ham_c, e_full).astype(BF)
    hg_col = by_lead(he_col, lead_gamma)

    panel = lax.all_gather(rho_t.reshape(2, cols, rows), "mode", axis=1, tiled=True)
    ham2_all = lax.all_gather(ham2_ct, "mode", axis=0, tiled=True)
    pi_b = auxiliary.astype(BF).reshape(rows, modes * 2 * coupled)
    pi_all = lax.all_gather(pi_b, "row", axis=0, tiled=True)

    onehot = (lead_index[:, None] == jnp.arange(leads, dtype=jnp.int32)[None, :]).astype(F32)
    lam_re, lam_im = -mode_width, mode_level
    l_parts, m_parts = [[], []], [[], []]
    for l in range(leads):
        s = [sum(onehot[k, l] * auxiliary[:, k, p] for k in range(modes)) for p in range(2)]
        m_re = sum(onehot[k, l] * (lam_re[k] * auxiliary[:, k, 0] - lam_im[k] * auxiliary[:, k, 1]) for k in range(modes))
        m_im = sum(onehot[k, l] * (lam_re[k] * auxiliary[:, k, 1] + lam_im[k] * auxiliary[:, k, 0]) for k in range(modes))
        for p in range(2):
            l_parts[p].append(s[p])
        m_parts[0].append(m_re)
        m_parts[1].append(m_im)
    l_part = jnp.concatenate(l_parts[0] + l_parts[1], axis=1)
    m_part = jnp.concatenate(m_parts[0] + m_parts[1], axis=1)
    w_l = jnp.concatenate([(residue[:, p][:, None] * onehot).sum(0) for p in range(2)])
    v_l = jnp.concatenate([((residue[:, p] * occupation)[:, None] * onehot).sum(0) for p in range(2)])

    hrho_b = hrho_t.astype(BF)
    f_re = dot(jnp.concatenate([hrho_b[cols:], rho_t[cols:]], 0), jnp.concatenate([2 * g_col, -hg_col.astype(BF)], 0), 0, 0)
    f_im = dot(jnp.concatenate([hrho_b[:cols], rho_t[:cols]], 0), jnp.concatenate([-2 * g_col, hg_col.astype(BF)], 0), 0, 0)
    f_part = jnp.concatenate([f_re, f_im], axis=1)
    l_part_b = l_part.astype(BF)
    n_part = jnp.concatenate([dot(l_part_b[:, :q], g_row, 0, 0), -dot(l_part_b[:, q:], g_row, 0, 0)], axis=1)

    piece = rows // n_mode
    n_piece = q // n_mode
    scal = jnp.concatenate([w_l, v_l])
    scal = jnp.zeros((n_mode, 1, 2 * q), F32).at[:, 0, : scal.shape[0]].set(scal)
    payload = jnp.concatenate(
        [a.reshape(n_mode, -1, 2 * q) for a in (l_part, m_part, f_part, n_part)] + [scal], axis=1
    )
    mine = lax.psum_scatter(payload, "mode", scatter_dimension=0, tiled=True)[0]
    n_mine = over_row(mine[3 * piece : 3 * piece + n_piece]).sum(0)
    w_sum, v_sum = mine[-1, : 2 * leads], mine[-1, 2 * leads : 4 * leads]
    mine = jnp.concatenate([mine[: 3 * piece], n_mine], axis=0).astype(BF)
    whole = lax.all_gather(mine, "mode", axis=0, tiled=False)
    l1_b = whole[:, :piece].reshape(rows, 2 * q)
    m1 = whole[:, piece : 2 * piece].reshape(rows, 2 * q).astype(F32)
    f_all = whole[:, 2 * piece : 3 * piece].reshape(rows, 2 * q).astype(F32)
    n_all = whole[:, 3 * piece :].reshape(q, 2 * q)

    grow_full = by_lead(e_full, lead_gamma).astype(BF)
    src = jnp.concatenate([dot(panel[p], grow_full, 0, 0) for p in range(2)], axis=1)
    w_q = jnp.repeat(w_sum, coupled)
    v_q = jnp.repeat(v_sum, coupled)
    s_re, s_im = src[:, :q], src[:, q:]
    g_row_f = g_row.astype(F32)
    drive = jnp.concatenate(
        [w_q[:q] * s_re - w_q[q:] * s_im - (v_q[:q] - v_q[q:]) * g_row_f, w_q[:q] * s_im + w_q[q:] * s_re - (v_q[:q] + v_q[q:]) * g_row_f], axis=1
    )
    x_row = (3.0 * l1_b.astype(F32) + 2 * H2 * (m1 + drive)).astype(BF)
    p1 = jnp.concatenate([dot(e_col, l1_b[:, p * q : (p + 1) * q], 1, 1) for p in range(2)], 0)
    xe = jnp.concatenate([dot(e_col, x_row[:, p * q : (p + 1) * q], 1, 1) for p in range(2)], 0)
    rhoh_t = jnp.concatenate([dot(ham_c, panel[p]) for p in range(2)], 0)
    y = hrho_t - 2.0 * rhoh_t + 2.0 * jnp.concatenate([-p1[cols:], p1[:cols]], 0)
    z = dot(lax.dynamic_slice_in_dim(ham_c, row_start, rows, 1), l1_b)
    owner = col_start // rows
    own_l = lax.dynamic_slice_in_dim(l1_b, col_start - owner * rows, cols, 0)
    own_x = lax.dynamic_slice_in_dim(x_row, col_start - owner * rows, cols, 0)
    mask = (x_pos == owner).astype(BF)
    second = over_row(jnp.concatenate([y.astype(BF), ham2_ct], 0))
    second = jnp.moveaxis(second, 0, 1).reshape(3 * cols, n)
    third = over_row(jnp.concatenate([z.astype(BF), own_l * mask, own_x * mask], 0)).astype(F32).sum(0)
    z, l_c, x_c = third[:cols], third[cols : 2 * cols], third[2 * cols :]
    hy = dot(second[: 2 * cols], hamiltonian, 1, 1)
    ham2_c = second[2 * cols :]
    rhoh2_t = jnp.concatenate([dot(ham2_c, panel[p]) for p in range(2)], 0)
    b_re = x_c[:, :q] + 4 * H2 * z[:, q:]
    b_im = -x_c[:, q:] + 4 * H2 * z[:, :q]
    back_re = dot(b_re.astype(BF), e_row, 1, 1)
    back_im = dot(b_im.astype(BF), e_row, 1, 1)
    l_cb = l_c.astype(BF)
    he_row_b = he_row.astype(BF)
    c1_re, c1_im = dot(l_cb[:, :q], he_row_b, 1, 1), -dot(l_cb[:, q:], he_row_b, 1, 1)
    c2_re, c2_im = dot(he_col, l1_b[:, :q], 1, 1), dot(he_col, l1_b[:, q:], 1, 1)
    d_re, d_im = c1_re - c2_re, c1_im - c2_im
    comm = hrho_t - rhoh_t
    base = -2 * H2 * (hy + rhoh2_t) + xe
    out_re = 3.0 * comm[cols:] + base[:cols] + back_re + 2 * H2 * d_im
    out_im = -3.0 * comm[:cols] + base[cols:] + back_im - 2 * H2 * d_re
    density_rate = jnp.swapaxes(jnp.stack([out_re, out_im]), 1, 2)

    h_pi = dot(hamiltonian, pi_all).reshape(rows, modes, 2, coupled)
    h2_pi = dot(ham2_all, pi_all.reshape(n, -1), 0, 0).reshape(rows, modes, 2, coupled)
    lg = jnp.concatenate([by_lead(l1_b[:, p * q : (p + 1) * q], lead_gamma) for p in range(2)], 1)
    u = 2 * H2 * (f_all + lg + dot(e_row, n_all))
    outs = []
    for k in range(modes):
        is0 = onehot[k, 0] > 0

        def pick(a):
            return jnp.where(is0, a[:, :coupled], a[:, coupled:])

        lr, li = lam_re[k], lam_im[k]
        wr, wi, occ = residue[k, 0], residue[k, 1], occupation[k]
        sr, si, ur, ui = pick(s_re), pick(s_im), pick(u[:, :q]), pick(u[:, q:])
        gk, hgk = pick(g_row_f), pick(hg_row)
        br, bi = sr - occ * gk, si - occ * gk
        ar, ai = 3 + 2 * H2 * lr, 2 * H2 * li
        tr = ar * br - ai * bi + ur - 2 * H2 * occ * hgk
        ti = ar * bi + ai * br + ui + 2 * H2 * occ * hgk
        pr, pim = auxiliary[:, k, 0], auxiliary[:, k, 1]
        cr = 3 * lr + 2 * H2 * (lr * lr - li * li)
        ci = 3 * li + 4 * H2 * lr * li
        er, ei = 4 * H2 * li, -3 - 4 * H2 * lr
        hr, hi = h_pi[:, k, 0], h_pi[:, k, 1]
        outs.append(cr * pr - ci * pim + er * hr - ei * hi - 2 * H2 * h2_pi[:, k, 0] + wr * tr - wi * ti)
        outs.append(cr * pim + ci * pr + er * hi + ei * hr - 2 * H2 * h2_pi[:, k, 1] + wr * ti + wi * tr)
    auxiliary_rate = jnp.stack(outs, axis=1).reshape(rows, modes, 2, coupled)
    return density_rate, auxiliary_rate


def solution(mesh):
    in_specs = (
        P(None, "row", "mode"),
        P("row", "mode", None, None),
        P("row", None),
        P(),
        P("mode"),
        P("mode"),
        P("mode"),
        P("mode", None),
        P("mode"),
        P(),
    )
    out_specs = (P(None, "row", "mode"), P("row", "mode", None, None))
    return jax.shard_map(shards, mesh=mesh, in_specs=in_specs, out_specs=out_specs, check_vma=False)
```

```python
import jax
import jax.numpy as jnp
from jax import lax
from jax.experimental import pallas as pl
from jax.experimental.pallas import tpu as pltpu
from jax.sharding import PartitionSpec as P

H2 = 0.05
F32 = jnp.float32
BF = jnp.bfloat16


def dot(a, b, ca=1, cb=0):
    return lax.dot_general(a, b, (((ca,), (cb,)), ((), ())), preferred_element_type=F32)


MESH = pl.DeviceIdType.MESH
NY, NZ = 4, 8


class Net:
    def __init__(self, send, recv):
        self.send, self.recv, self.used, self.sent = send, recv, 0, []
        m = lax.axis_index("mode")
        self.x = lax.axis_index("row")
        self.c, self.z, self.y = lax.rem(m, 2), lax.rem(m // 2, NZ), m // (2 * NZ)

    def dev(self, y=None, z=None, c=None, x=None):
        y = self.y if y is None else y
        z = self.z if z is None else z
        c = self.c if c is None else c
        return {"mode": (y * NZ + z) * 2 + c, "row": self.x if x is None else x}

    def at(self, name, d):
        size = {"x": 4, "y": NY, "z": NZ}[name]
        return lax.rem(getattr(self, name) + (d % size), size)

    def slot(self):
        self.used += 1
        return self.used - 1

    def start(self, src, dst, to, slot):
        copy = pltpu.make_async_remote_copy(
            src_ref=src, dst_ref=dst, send_sem=self.send.at[slot], recv_sem=self.recv.at[slot], device_id=to, device_id_type=MESH
        )
        copy.start()
        self.sent.append(copy)

    def arrive(self, ref, slot):
        pltpu.make_async_remote_copy(
            src_ref=ref, dst_ref=ref, send_sem=self.send.at[slot], recv_sem=self.recv.at[slot],
            device_id=self.dev(c=1 - self.c), device_id_type=MESH,
        ).wait_recv()

    def finish(self):
        for copy in self.sent:
            copy.wait_send()

    def greet(self, peers):
        barrier = pltpu.get_barrier_semaphore()
        for peer in peers:
            pl.semaphore_signal(barrier, inc=1, device_id=peer, device_id_type=MESH)
        pl.semaphore_wait(barrier, len(peers))


def ring(net, name, part, share, t, step):
    size = {"x": 4, "y": NY, "z": NZ}[name]
    far = size // 2
    slots = {(d, s): net.slot() for s in range(1, far + 1) for d in (1, -1)}
    at = lambda d: net.at(name, d)
    for d in (1, -1):
        net.start(part(at(0), None), part(at(0), None), net.dev(**{name: at(d)}), slots[d, 1])
    share(at(0))
    for s in range(1, far + 1):
        yield t + s * step
        for d in (1, -1):
            half = None if s < far else (d + 1) // 2
            net.arrive(part(at(-d * s), half), slots[d, s])
            if s < far:
                half = None if s + 1 < far else (d + 1) // 2
                net.start(part(at(-d * s), half), part(at(-d * s), half), net.dev(**{name: at(d)}), slots[d, s + 1])
        if s < far:
            share(at(s))
            share(at(-s))
        else:
            share(at(far))


def gather_plane(net, buf, cut, rows, lanes, t, unit):
    lane = {None: pl.ds(0, lanes), 0: pl.ds(0, lanes // 2), 1: pl.ds(lanes // 2, lanes // 2)}
    low, high = pl.ds(0, cut), pl.ds(cut, rows - cut)
    c = net.c
    waits = []

    def share_of(ref_of):
        def share(pos):
            slot = net.slot()
            mine, theirs = ref_of(pos, c), ref_of(pos, 1 - c)
            net.start(mine, mine, net.dev(c=1 - c), slot)
            waits.append((theirs, slot))
        return share

    def nothing(pos):
        pass

    def first():
        yield from ring(net, "y", lambda p, h: buf.at[p, net.z, c, low, lane[h]], nothing, t, 2.0 + unit)
        yield from ring(
            net, "z", lambda p, h: buf.at[:, p, c, low, lane[h]],
            share_of(lambda p, cc: buf.at[:, p, cc, low, lane[None]]), t + 5.0 + 2 * unit, 2.0 + 4 * unit,
        )

    def second():
        yield from ring(net, "z", lambda p, h: buf.at[net.y, p, c, high, lane[h]], nothing, t, 2.0 + unit)
        yield from ring(
            net, "y", lambda p, h: buf.at[p, :, c, high, lane[h]],
            share_of(lambda p, cc: buf.at[p, :, cc, high, lane[None]]), t + 9.0 + 4 * unit, 2.0 + 8 * unit,
        )

    yield from merge([first(), second()])
    yield t + 12.0 + 30 * unit
    for ref, slot in waits:
        net.arrive(ref, slot)


def merge(threads):
    live = []
    for thread in threads:
        when = next(thread, None)
        if when is not None:
            live.append([when, len(live), thread])
    while live:
        live.sort(key=lambda item: (item[0], item[1]))
        yield live[0][0]
        when = next(live[0][2], None)
        if when is None:
            live.pop(0)
        else:
            live[0][0] = when


def reduce_plane(net, pay, whole, pair, acc, got1, got2, gotz, xs_out, xs_in, keep_rows):
    c, y, z = net.c, net.y, net.z
    slot = net.slot()
    net.start(pay.at[1 - c], pair, net.dev(c=1 - c), slot)
    yield 3.0
    net.arrive(pair, slot)

    def add_pair(i, carry):
        acc[i] = (pay[c, i].astype(F32) + pair[i].astype(F32)).astype(BF)
        return carry

    lax.fori_loop(0, NY, add_pair, 0)
    near, over = y + 1 - 2 * lax.rem(y, 2), NY - 1 - y
    half = NZ // 2
    colors = []
    for color, (f, s) in enumerate(((near, over), (over, near))):
        s_of_f = lax.rem(y + 2, NY)
        zs = pl.ds(color * half, half)
        slots = [net.slot() for _ in range(3)]
        net.start(acc.at[f, zs], got1.at[color, 0], net.dev(y=f), slots[0])
        net.start(acc.at[s_of_f, zs], got1.at[color, 1], net.dev(y=f), slots[1])
        colors.append((f, s, zs, slots))
    yield 10.0
    for color, (f, s, zs, slots) in enumerate(colors):
        net.arrive(got1.at[color, 1], slots[1])
        acc[s, zs] = (acc[s, zs].astype(F32) + got1[color, 1].astype(F32)).astype(BF)
        net.start(acc.at[s, zs], got2.at[color], net.dev(y=s), slots[2])
    yield 15.0
    for color, (f, s, zs, slots) in enumerate(colors):
        net.arrive(got1.at[color, 0], slots[0])
        net.arrive(got2.at[color], slots[2])
        acc[y, zs] = (acc[y, zs].astype(F32) + got1[color, 0].astype(F32) + got2[color].astype(F32)).astype(BF)
    zslots = [net.slot() for _ in range(NZ - 1)]
    for d in (4, 3, 5, 2, 6, 1, 7):
        net.start(acc.at[y, net.at("z", d)], gotz.at[d - 1], net.dev(z=net.at("z", d)), zslots[d - 1])
    yield 23.0
    total = acc[y, z].astype(F32)
    for d in range(1, NZ):
        net.arrive(gotz.at[d - 1], zslots[d - 1])
        total = total + gotz[d - 1].astype(F32)
    xs_out[...] = total[keep_rows:]
    xslots = [net.slot() for _ in range(3)]
    for d in (1, 2, 3):
        net.start(xs_out, xs_in.at[d - 1], net.dev(x=net.at("x", d)), xslots[d - 1])
    yield 26.0
    tail = total[keep_rows:]
    for d in (1, 2, 3):
        net.arrive(xs_in.at[d - 1], xslots[d - 1])
    summed = tail + xs_in[0] + xs_in[1] + xs_in[2]
    index = lax.broadcasted_iota(jnp.int32, tail.shape, 0)
    tail = jnp.where(index < tail.shape[0] // 2, summed, tail)
    whole[y, z, c] = jnp.concatenate([total[:keep_rows], tail], axis=0).astype(BF)
    yield from gather_plane(net, whole, 16, 32, whole.shape[-1], 27.0, 0.35)


def gather_rows(net, pi, pall):
    rows = pi.shape[0] // 2
    halves = (pl.ds(0, rows), pl.ds(rows, rows))
    x = net.x
    slots = {(d, i): net.slot() for d in (0, 1) for i in range(3)}
    for i in (0, 1):
        for d, way in ((0, 1), (1, -1)):
            h = halves[i if d == 0 else 1 - i]
            net.start(pi.at[h], pall.at[x, h], net.dev(x=net.at("x", way)), slots[d, i])
    pall[x] = pi[...]
    yield 13.0
    for d, way in ((0, 1), (1, -1)):
        ref = pall.at[net.at("x", -way), halves[d]]
        net.arrive(ref, slots[d, 0])
        net.start(ref, ref, net.dev(x=net.at("x", way)), slots[d, 2])
    yield 36.0
    for d, way in ((0, 1), (1, -1)):
        net.arrive(pall.at[net.at("x", -way), halves[1 - d]], slots[d, 1])
        net.arrive(pall.at[net.at("x", -2), halves[d]], slots[d, 2])


def main_kernel(pi, blk, pay, pall, panel, whole, pair, acc, got1, got2, gotz, xs_out, xs_in, send, recv):
    net = Net(send, recv)
    peers = [net.dev(x=net.at("x", d)) for d in (1, 2, 3)]
    peers += [net.dev(y=net.at("y", d)) for d in (1, 3)]
    peers += [net.dev(z=net.at("z", d)) for d in range(1, NZ)]
    peers += [net.dev(c=1 - net.c)]
    net.greet(peers)
    panel[net.y, net.z, net.c] = blk[...]
    rows, lanes = blk.shape

    def planes():
        yield from gather_plane(net, panel, rows // 2, rows, lanes, 1.0, 1.1)

    for _ in merge([
        reduce_plane(net, pay, whole, pair, acc, got1, got2, gotz, xs_out, xs_in, 24),
        gather_rows(net, pi, pall),
        planes(),
    ]):
        pass
    net.finish()


def exchange(pi, blk, pay):
    rows, lanes = blk.shape
    vm = pl.BlockSpec(memory_space=pltpu.VMEM)
    sems = 128
    return pl.pallas_call(
        main_kernel,
        out_shape=[
            jax.ShapeDtypeStruct((4, *pi.shape), BF),
            jax.ShapeDtypeStruct((NY, NZ, 2, rows, lanes), BF),
            jax.ShapeDtypeStruct((NY, NZ, 2, 32, lanes), BF),
        ],
        in_specs=[vm] * 3,
        out_specs=[vm] * 3,
        scratch_shapes=[
            pltpu.VMEM((NY, NZ, 32, lanes), BF),
            pltpu.VMEM((NY, NZ, 32, lanes), BF),
            pltpu.VMEM((2, 2, NZ // 2, 32, lanes), BF),
            pltpu.VMEM((2, NZ // 2, 32, lanes), BF),
            pltpu.VMEM((NZ - 1, 32, lanes), BF),
            pltpu.VMEM((8, lanes), F32),
            pltpu.VMEM((3, 8, lanes), F32),
            pltpu.SemaphoreType.DMA((sems,)),
            pltpu.SemaphoreType.DMA((sems,)),
        ],
        compiler_params=pltpu.CompilerParams(collective_id=1, has_side_effects=True, vmem_limit_bytes=48 * 1024 * 1024),
        name="exchange",
    )(pi, blk, pay)


def rows_kernel(blk, out, send, recv):
    net = Net(send, recv)
    net.greet([net.dev(x=net.at("x", d)) for d in (1, 2, 3)])
    slots = [net.slot() for _ in range(3)]
    lanes = blk.shape[1]

    def place(x):
        return out.at[:, pl.ds(pl.multiple_of(x * lanes, lanes), lanes)]

    for d in (2, 1, 3):
        net.start(blk, place(net.x), net.dev(x=net.at("x", d)), slots[d - 1])
    out[:, pl.ds(pl.multiple_of(net.x * lanes, lanes), lanes)] = blk[...]
    for d in (1, 3, 2):
        net.arrive(place(net.at("x", -d)), slots[d - 1])
    net.finish()


def over_row(blk, ident):
    vm = pl.BlockSpec(memory_space=pltpu.VMEM)
    return pl.pallas_call(
        rows_kernel,
        out_shape=jax.ShapeDtypeStruct((blk.shape[0], 4 * blk.shape[1]), blk.dtype),
        in_specs=[vm],
        out_specs=vm,
        scratch_shapes=[pltpu.SemaphoreType.DMA((3,)), pltpu.SemaphoreType.DMA((3,))],
        compiler_params=pltpu.CompilerParams(collective_id=ident, has_side_effects=True, vmem_limit_bytes=4 * 1024 * 1024),
        name="rows",
    )(blk)


def by_lead(x, gamma):
    leads, coupled = gamma.shape[:2]
    return jnp.concatenate(
        [dot(x[:, l * coupled : (l + 1) * coupled], gamma[l]) for l in range(leads)], axis=1
    )


def shards(density, auxiliary, hamiltonian, coupling, lead_index, mode_level, mode_width, residue, occupation, lead_gamma):
    rows, cols = density.shape[1:]
    n = hamiltonian.shape[1]
    leads, coupled = coupling.shape
    q = leads * coupled
    modes = auxiliary.shape[1]
    n_mode = lax.axis_size("mode")
    n_row = lax.axis_size("row")
    x_pos, m_pos = lax.axis_index("row"), lax.axis_index("mode")
    row_start, col_start = x_pos * rows, m_pos * cols
    flat = coupling.reshape(-1)

    e_full = (jnp.arange(n, dtype=jnp.int32)[:, None] == flat[None, :]).astype(BF)
    e_row = (row_start + jnp.arange(rows, dtype=jnp.int32)[:, None] == flat[None, :]).astype(BF)
    e_col = (col_start + jnp.arange(cols, dtype=jnp.int32)[:, None] == flat[None, :]).astype(BF)
    g_row = by_lead(e_row, lead_gamma).astype(BF)
    g_col = by_lead(e_col, lead_gamma).astype(BF)

    rho_t = jnp.swapaxes(density, 1, 2).astype(BF).reshape(2 * cols, rows)
    ham_ct = jnp.swapaxes(lax.dynamic_slice_in_dim(hamiltonian, col_start, cols, 1), 0, 1)

    first = over_row(jnp.concatenate([ham_ct, rho_t], axis=0), 2)
    ham_c = first[:cols]
    applied = dot(first, hamiltonian, 1, 1)
    ham2_ct = applied[:cols].astype(BF)
    hrho_t = applied[cols:]
    he_row = dot(hamiltonian, e_full)
    hg_row = by_lead(he_row.astype(BF), lead_gamma)
    he_col = dot(ham_c, e_full).astype(BF)
    hg_col = by_lead(he_col, lead_gamma)

    pi_b = auxiliary.astype(BF).reshape(rows, modes * 2 * coupled)

    onehot = (lead_index[:, None] == jnp.arange(leads, dtype=jnp.int32)[None, :]).astype(F32)
    lam_re, lam_im = -mode_width, mode_level
    l_parts, m_parts = [[], []], [[], []]
    for l in range(leads):
        s = [sum(onehot[k, l] * auxiliary[:, k, p] for k in range(modes)) for p in range(2)]
        m_re = sum(onehot[k, l] * (lam_re[k] * auxiliary[:, k, 0] - lam_im[k] * auxiliary[:, k, 1]) for k in range(modes))
        m_im = sum(onehot[k, l] * (lam_re[k] * auxiliary[:, k, 1] + lam_im[k] * auxiliary[:, k, 0]) for k in range(modes))
        for p in range(2):
            l_parts[p].append(s[p])
        m_parts[0].append(m_re)
        m_parts[1].append(m_im)
    l_part = jnp.concatenate(l_parts[0] + l_parts[1], axis=1)
    m_part = jnp.concatenate(m_parts[0] + m_parts[1], axis=1)
    w_l = jnp.concatenate([(residue[:, p][:, None] * onehot).sum(0) for p in range(2)])
    v_l = jnp.concatenate([((residue[:, p] * occupation)[:, None] * onehot).sum(0) for p in range(2)])

    hrho_b = hrho_t.astype(BF)
    f_re = dot(jnp.concatenate([hrho_b[cols:], rho_t[cols:]], 0), jnp.concatenate([2 * g_col, -hg_col.astype(BF)], 0), 0, 0)
    f_im = dot(jnp.concatenate([hrho_b[:cols], rho_t[:cols]], 0), jnp.concatenate([-2 * g_col, hg_col.astype(BF)], 0), 0, 0)
    f_part = jnp.concatenate([f_re, f_im], axis=1)
    l_part_b = l_part.astype(BF)
    n_part = jnp.concatenate([dot(l_part_b[:, :q], g_row, 0, 0), -dot(l_part_b[:, q:], g_row, 0, 0)], axis=1)

    piece = rows // n_mode
    n_piece = q // n_mode
    scal = jnp.concatenate([w_l, v_l])
    scal = jnp.zeros((n_mode, 4, 2 * q), F32).at[:, 0, : scal.shape[0]].set(scal)
    payload = jnp.concatenate(
        [a.reshape(n_mode, -1, 2 * q) for a in (l_part, m_part, f_part, n_part)] + [scal], axis=1
    ).astype(BF)
    payload = payload.reshape(NY, NZ, 2, 32, 2 * q).transpose(2, 0, 1, 3, 4)
    pi_all, panel, whole = exchange(pi_b, jnp.concatenate([rho_t, ham2_ct], 0), payload)
    pi_all = pi_all.reshape(n, -1)
    panel = panel.reshape(n_mode, 3, cols, rows)
    ham2_all = panel[:, 2].reshape(n, rows)
    panel = [panel[:, p].reshape(n, rows) for p in range(2)]
    whole = whole.reshape(n_mode, 32, 2 * q)
    l1_b = whole[:, :piece].reshape(rows, 2 * q)
    m1 = whole[:, piece : 2 * piece].reshape(rows, 2 * q).astype(F32)
    f_all = whole[:, 2 * piece : 3 * piece].reshape(rows, 2 * q).astype(F32)
    n_all = whole[:, 3 * piece : 3 * piece + n_piece].reshape(q, 2 * q)
    scal = whole[0, 3 * piece + n_piece].astype(F32)
    w_sum, v_sum = scal[: 2 * leads], scal[2 * leads : 4 * leads]

    grow_full = by_lead(e_full, lead_gamma).astype(BF)
    src = jnp.concatenate([dot(panel[p], grow_full, 0, 0) for p in range(2)], axis=1)
    w_q = jnp.repeat(w_sum, coupled)
    v_q = jnp.repeat(v_sum, coupled)
    s_re, s_im = src[:, :q], src[:, q:]
    g_row_f = g_row.astype(F32)
    drive = jnp.concatenate(
        [w_q[:q] * s_re - w_q[q:] * s_im - (v_q[:q] - v_q[q:]) * g_row_f, w_q[:q] * s_im + w_q[q:] * s_re - (v_q[:q] + v_q[q:]) * g_row_f], axis=1
    )
    x_row = (3.0 * l1_b.astype(F32) + 2 * H2 * (m1 + drive)).astype(BF)
    p1 = jnp.concatenate([dot(e_col, l1_b[:, p * q : (p + 1) * q], 1, 1) for p in range(2)], 0)
    xe = jnp.concatenate([dot(e_col, x_row[:, p * q : (p + 1) * q], 1, 1) for p in range(2)], 0)
    rhoh_t = jnp.concatenate([dot(ham_c, panel[p]) for p in range(2)], 0)
    y = hrho_t - 2.0 * rhoh_t + 2.0 * jnp.concatenate([-p1[cols:], p1[:cols]], 0)
    z = dot(lax.dynamic_slice_in_dim(ham_c, row_start, rows, 1), l1_b)
    owner = col_start // rows
    own_l = lax.dynamic_slice_in_dim(l1_b, col_start - owner * rows, cols, 0)
    own_x = lax.dynamic_slice_in_dim(x_row, col_start - owner * rows, cols, 0)
    mask = (x_pos == owner).astype(BF)
    second = over_row(jnp.concatenate([y.astype(BF), ham2_ct, z.astype(BF), own_l * mask, own_x * mask], 0), 3)
    third = second[3 * cols :].astype(F32)
    third = sum(third[:, i * rows : (i + 1) * rows] for i in range(n_row))
    z, l_c, x_c = third[:cols], third[cols : 2 * cols], third[2 * cols :]
    hy = dot(second[: 2 * cols], hamiltonian, 1, 1)
    ham2_c = second[2 * cols : 3 * cols]
    rhoh2_t = jnp.concatenate([dot(ham2_c, panel[p]) for p in range(2)], 0)
    b_re = x_c[:, :q] + 4 * H2 * z[:, q:]
    b_im = -x_c[:, q:] + 4 * H2 * z[:, :q]
    back_re = dot(b_re.astype(BF), e_row, 1, 1)
    back_im = dot(b_im.astype(BF), e_row, 1, 1)
    l_cb = l_c.astype(BF)
    he_row_b = he_row.astype(BF)
    c1_re, c1_im = dot(l_cb[:, :q], he_row_b, 1, 1), -dot(l_cb[:, q:], he_row_b, 1, 1)
    c2_re, c2_im = dot(he_col, l1_b[:, :q], 1, 1), dot(he_col, l1_b[:, q:], 1, 1)
    d_re, d_im = c1_re - c2_re, c1_im - c2_im
    comm = hrho_t - rhoh_t
    base = -2 * H2 * (hy + rhoh2_t) + xe
    out_re = 3.0 * comm[cols:] + base[:cols] + back_re + 2 * H2 * d_im
    out_im = -3.0 * comm[:cols] + base[cols:] + back_im - 2 * H2 * d_re
    density_rate = jnp.swapaxes(jnp.stack([out_re, out_im]), 1, 2)

    h_pi = dot(hamiltonian, pi_all).reshape(rows, modes, 2, coupled)
    h2_pi = dot(ham2_all, pi_all.reshape(n, -1), 0, 0).reshape(rows, modes, 2, coupled)
    lg = jnp.concatenate([by_lead(l1_b[:, p * q : (p + 1) * q], lead_gamma) for p in range(2)], 1)
    u = 2 * H2 * (f_all + lg + dot(e_row, n_all))
    outs = []
    for k in range(modes):
        is0 = onehot[k, 0] > 0

        def pick(a):
            return jnp.where(is0, a[:, :coupled], a[:, coupled:])

        lr, li = lam_re[k], lam_im[k]
        wr, wi, occ = residue[k, 0], residue[k, 1], occupation[k]
        sr, si, ur, ui = pick(s_re), pick(s_im), pick(u[:, :q]), pick(u[:, q:])
        gk, hgk = pick(g_row_f), pick(hg_row)
        br, bi = sr - occ * gk, si - occ * gk
        ar, ai = 3 + 2 * H2 * lr, 2 * H2 * li
        tr = ar * br - ai * bi + ur - 2 * H2 * occ * hgk
        ti = ar * bi + ai * br + ui + 2 * H2 * occ * hgk
        pr, pim = auxiliary[:, k, 0], auxiliary[:, k, 1]
        cr = 3 * lr + 2 * H2 * (lr * lr - li * li)
        ci = 3 * li + 4 * H2 * lr * li
        er, ei = 4 * H2 * li, -3 - 4 * H2 * lr
        hr, hi = h_pi[:, k, 0], h_pi[:, k, 1]
        outs.append(cr * pr - ci * pim + er * hr - ei * hi - 2 * H2 * h2_pi[:, k, 0] + wr * tr - wi * ti)
        outs.append(cr * pim + ci * pr + er * hi + ei * hr - 2 * H2 * h2_pi[:, k, 1] + wr * ti + wi * tr)
    auxiliary_rate = jnp.stack(outs, axis=1).reshape(rows, modes, 2, coupled)
    return density_rate, auxiliary_rate


def solution(mesh):
    in_specs = (
        P(None, "row", "mode"),
        P("row", "mode", None, None),
        P("row", None),
        P(),
        P("mode"),
        P("mode"),
        P("mode"),
        P("mode", None),
        P("mode"),
        P(),
    )
    out_specs = (P(None, "row", "mode"), P("row", "mode", None, None))
    return jax.shard_map(shards, mesh=mesh, in_specs=in_specs, out_specs=out_specs, check_vma=False)
```

```python
import jax
import jax.numpy as jnp
from jax import lax
from jax.experimental import pallas as pl
from jax.experimental.pallas import tpu as pltpu
from jax.sharding import PartitionSpec as P

H2 = 0.05
F32 = jnp.float32
BF = jnp.bfloat16


def dot(a, b, ca=1, cb=0):
    return lax.dot_general(a, b, (((ca,), (cb,)), ((), ())), preferred_element_type=F32)


MESH = pl.DeviceIdType.MESH
NY, NZ = 4, 8


class Net:
    def __init__(self, send, recv):
        self.send, self.recv, self.used, self.sent = send, recv, 0, []
        m = lax.axis_index("mode")
        self.x = lax.axis_index("row")
        self.c, self.z, self.y = lax.rem(m, 2), lax.rem(m // 2, NZ), m // (2 * NZ)

    def dev(self, y=None, z=None, c=None, x=None):
        y = self.y if y is None else y
        z = self.z if z is None else z
        c = self.c if c is None else c
        return {"mode": (y * NZ + z) * 2 + c, "row": self.x if x is None else x}

    def at(self, name, d):
        size = {"x": 4, "y": NY, "z": NZ}[name]
        return lax.rem(getattr(self, name) + (d % size), size)

    def slot(self):
        self.used += 1
        return self.used - 1

    def start(self, src, dst, to, slot):
        copy = pltpu.make_async_remote_copy(
            src_ref=src, dst_ref=dst, send_sem=self.send.at[slot], recv_sem=self.recv.at[slot], device_id=to, device_id_type=MESH
        )
        copy.start()
        self.sent.append(copy)

    def arrive(self, ref, slot):
        pltpu.make_async_remote_copy(
            src_ref=ref, dst_ref=ref, send_sem=self.send.at[slot], recv_sem=self.recv.at[slot],
            device_id=self.dev(c=1 - self.c), device_id_type=MESH,
        ).wait_recv()

    def finish(self):
        for copy in self.sent:
            copy.wait_send()

    def greet(self, peers):
        barrier = pltpu.get_barrier_semaphore()
        for peer in peers:
            pl.semaphore_signal(barrier, inc=1, device_id=peer, device_id_type=MESH)
        pl.semaphore_wait(barrier, len(peers))


def ring(net, name, part, share, t, step):
    size = {"x": 4, "y": NY, "z": NZ}[name]
    far = size // 2
    slots = {(d, s): net.slot() for s in range(1, far + 1) for d in (1, -1)}
    at = lambda d: net.at(name, d)
    for d in (1, -1):
        net.start(part(at(0), None), part(at(0), None), net.dev(**{name: at(d)}), slots[d, 1])
    share(at(0))
    for s in range(1, far + 1):
        yield t + s * step
        for d in (1, -1):
            half = None if s < far else (d + 1) // 2
            net.arrive(part(at(-d * s), half), slots[d, s])
            if s < far:
                half = None if s + 1 < far else (d + 1) // 2
                net.start(part(at(-d * s), half), part(at(-d * s), half), net.dev(**{name: at(d)}), slots[d, s + 1])
        if s < far:
            share(at(s))
            share(at(-s))
        else:
            share(at(far))


def gather_plane(net, buf, cut, rows, lanes, t, unit):
    lane = {None: pl.ds(0, lanes), 0: pl.ds(0, lanes // 2), 1: pl.ds(lanes // 2, lanes // 2)}
    low, high = pl.ds(0, cut), pl.ds(cut, rows - cut)
    c = net.c
    waits = []

    def share_of(ref_of):
        def share(pos):
            slot = net.slot()
            mine, theirs = ref_of(pos, c), ref_of(pos, 1 - c)
            net.start(mine, mine, net.dev(c=1 - c), slot)
            waits.append((theirs, slot))
        return share

    def nothing(pos):
        pass

    def first():
        yield from ring(net, "y", lambda p, h: buf.at[p, net.z, c, low, lane[h]], nothing, t, 2.0 + unit)
        yield from ring(
            net, "z", lambda p, h: buf.at[:, p, c, low, lane[h]],
            share_of(lambda p, cc: buf.at[:, p, cc, low, lane[None]]), t + 5.0 + 2 * unit, 2.0 + 4 * unit,
        )

    def second():
        yield from ring(net, "z", lambda p, h: buf.at[net.y, p, c, high, lane[h]], nothing, t, 2.0 + unit)
        yield from ring(
            net, "y", lambda p, h: buf.at[p, :, c, high, lane[h]],
            share_of(lambda p, cc: buf.at[p, :, cc, high, lane[None]]), t + 9.0 + 4 * unit, 2.0 + 8 * unit,
        )

    yield from merge([first(), second()])
    yield t + 12.0 + 30 * unit
    for ref, slot in waits:
        net.arrive(ref, slot)


def merge(threads):
    live = []
    for thread in threads:
        when = next(thread, None)
        if when is not None:
            live.append([when, len(live), thread])
    while live:
        live.sort(key=lambda item: (item[0], item[1]))
        yield live[0][0]
        when = next(live[0][2], None)
        if when is None:
            live.pop(0)
        else:
            live[0][0] = when


def reduce_plane(net, pay, whole, pair, acc, got1, got2, gotz, xs_out, xs_in, keep_rows):
    c, y, z = net.c, net.y, net.z
    slot = net.slot()
    net.start(pay.at[1 - c], pair, net.dev(c=1 - c), slot)
    yield 3.0
    net.arrive(pair, slot)

    def add_pair(i, carry):
        acc[i] = (pay[c, i].astype(F32) + pair[i].astype(F32)).astype(BF)
        return carry

    lax.fori_loop(0, NY, add_pair, 0)
    near, over = y + 1 - 2 * lax.rem(y, 2), NY - 1 - y
    half = NZ // 2
    colors = []
    for color, (f, s) in enumerate(((near, over), (over, near))):
        s_of_f = lax.rem(y + 2, NY)
        zs = pl.ds(color * half, half)
        slots = [net.slot() for _ in range(3)]
        net.start(acc.at[f, zs], got1.at[color, 0], net.dev(y=f), slots[0])
        net.start(acc.at[s_of_f, zs], got1.at[color, 1], net.dev(y=f), slots[1])
        colors.append((f, s, zs, slots))
    yield 10.0
    for color, (f, s, zs, slots) in enumerate(colors):
        net.arrive(got1.at[color, 1], slots[1])
        acc[s, zs] = (acc[s, zs].astype(F32) + got1[color, 1].astype(F32)).astype(BF)
        net.start(acc.at[s, zs], got2.at[color], net.dev(y=s), slots[2])
    yield 15.0
    for color, (f, s, zs, slots) in enumerate(colors):
        net.arrive(got1.at[color, 0], slots[0])
        net.arrive(got2.at[color], slots[2])
        acc[y, zs] = (acc[y, zs].astype(F32) + got1[color, 0].astype(F32) + got2[color].astype(F32)).astype(BF)
    zslots = [net.slot() for _ in range(NZ - 1)]
    for d in (4, 3, 5, 2, 6, 1, 7):
        net.start(acc.at[y, net.at("z", d)], gotz.at[d - 1], net.dev(z=net.at("z", d)), zslots[d - 1])
    yield 23.0
    total = acc[y, z].astype(F32)
    for d in range(1, NZ):
        net.arrive(gotz.at[d - 1], zslots[d - 1])
        total = total + gotz[d - 1].astype(F32)
    xs_out[...] = total[keep_rows:]
    xslots = [net.slot() for _ in range(3)]
    for d in (1, 2, 3):
        net.start(xs_out, xs_in.at[d - 1], net.dev(x=net.at("x", d)), xslots[d - 1])
    yield 26.0
    tail = total[keep_rows:]
    for d in (1, 2, 3):
        net.arrive(xs_in.at[d - 1], xslots[d - 1])
    summed = tail + xs_in[0] + xs_in[1] + xs_in[2]
    tail = jnp.where(jnp.full(tail.shape, c) == 0, summed, tail)
    whole[y, z, c] = jnp.concatenate([total[:keep_rows], tail], axis=0).astype(BF)
    yield from gather_plane(net, whole, 16, 32, whole.shape[-1], 27.0, 0.35)


def gather_rows(net, pi, pall):
    rows = pi.shape[0] // 2
    halves = (pl.ds(0, rows), pl.ds(rows, rows))
    x = net.x
    slots = {(d, i): net.slot() for d in (0, 1) for i in range(3)}
    for i in (0, 1):
        for d, way in ((0, 1), (1, -1)):
            h = halves[i if d == 0 else 1 - i]
            net.start(pi.at[h], pall.at[x, h], net.dev(x=net.at("x", way)), slots[d, i])
    pall[x] = pi[...]
    yield 13.0
    for d, way in ((0, 1), (1, -1)):
        ref = pall.at[net.at("x", -way), halves[d]]
        net.arrive(ref, slots[d, 0])
        net.start(ref, ref, net.dev(x=net.at("x", way)), slots[d, 2])
    yield 36.0
    for d, way in ((0, 1), (1, -1)):
        net.arrive(pall.at[net.at("x", -way), halves[1 - d]], slots[d, 1])
        net.arrive(pall.at[net.at("x", -2), halves[d]], slots[d, 2])


def main_kernel(pi, blk, pay, pall, panel, whole, pair, acc, got1, got2, gotz, xs_out, xs_in, send, recv):
    net = Net(send, recv)
    peers = [net.dev(x=net.at("x", d)) for d in (1, 2, 3)]
    peers += [net.dev(y=net.at("y", d)) for d in (1, 3)]
    peers += [net.dev(z=net.at("z", d)) for d in range(1, NZ)]
    peers += [net.dev(c=1 - net.c)]
    net.greet(peers)
    panel[net.y, net.z, net.c] = blk[...]
    rows, lanes = blk.shape

    def planes():
        yield from gather_plane(net, panel, rows // 2, rows, lanes, 1.0, 1.1)

    for _ in merge([
        reduce_plane(net, pay, whole, pair, acc, got1, got2, gotz, xs_out, xs_in, 24),
        gather_rows(net, pi, pall),
        planes(),
    ]):
        pass
    net.finish()


def exchange(pi, blk, pay):
    rows, lanes = blk.shape
    vm = pl.BlockSpec(memory_space=pltpu.VMEM)
    sems = 128
    return pl.pallas_call(
        main_kernel,
        out_shape=[
            jax.ShapeDtypeStruct((4, *pi.shape), BF),
            jax.ShapeDtypeStruct((NY, NZ, 2, rows, lanes), BF),
            jax.ShapeDtypeStruct((NY, NZ, 2, 32, lanes), BF),
        ],
        in_specs=[vm] * 3,
        out_specs=[vm] * 3,
        scratch_shapes=[
            pltpu.VMEM((NY, NZ, 32, lanes), BF),
            pltpu.VMEM((NY, NZ, 32, lanes), BF),
            pltpu.VMEM((2, 2, NZ // 2, 32, lanes), BF),
            pltpu.VMEM((2, NZ // 2, 32, lanes), BF),
            pltpu.VMEM((NZ - 1, 32, lanes), BF),
            pltpu.VMEM((8, lanes), F32),
            pltpu.VMEM((3, 8, lanes), F32),
            pltpu.SemaphoreType.DMA((sems,)),
            pltpu.SemaphoreType.DMA((sems,)),
        ],
        compiler_params=pltpu.CompilerParams(collective_id=1, has_side_effects=True, vmem_limit_bytes=48 * 1024 * 1024),
        name="exchange",
    )(pi, blk, pay)


def rows_kernel(blk, out, send, recv):
    net = Net(send, recv)
    net.greet([net.dev(x=net.at("x", d)) for d in (1, 2, 3)])
    slots = [net.slot() for _ in range(3)]
    lanes = blk.shape[1]

    def place(x):
        return out.at[:, pl.ds(pl.multiple_of(x * lanes, lanes), lanes)]

    for d in (2, 1, 3):
        net.start(blk, place(net.x), net.dev(x=net.at("x", d)), slots[d - 1])
    out[:, pl.ds(pl.multiple_of(net.x * lanes, lanes), lanes)] = blk[...]
    for d in (1, 3, 2):
        net.arrive(place(net.at("x", -d)), slots[d - 1])
    net.finish()


def over_row(blk, ident):
    vm = pl.BlockSpec(memory_space=pltpu.VMEM)
    return pl.pallas_call(
        rows_kernel,
        out_shape=jax.ShapeDtypeStruct((blk.shape[0], 4 * blk.shape[1]), blk.dtype),
        in_specs=[vm],
        out_specs=vm,
        scratch_shapes=[pltpu.SemaphoreType.DMA((3,)), pltpu.SemaphoreType.DMA((3,))],
        compiler_params=pltpu.CompilerParams(collective_id=ident, has_side_effects=True, vmem_limit_bytes=4 * 1024 * 1024),
        name="rows",
    )(blk)


def sums_kernel(lead, coef, aux, f_re, f_im, g_row, pi, pay, held):
    q = g_row.shape[1]
    coupled = aux.shape[1]
    modes = aux.shape[0] // (2 * held.shape[0])
    leads = q // coupled
    hot = [[jnp.where(lead[k] == l, 1.0, 0.0) for l in range(leads)] for k in range(modes)]
    level, width, re, im, occ = ([coef[i, k] for k in range(modes)] for i in range(5))

    def chunk(t, carry):
        rows = pl.ds(pl.multiple_of(32 * t, 32), 32)
        part = [aux[pl.ds(pl.multiple_of(32 * t * 2 * modes, 32) + i, 32, stride=2 * modes), :] for i in range(2 * modes)]
        pi[rows, :] = jnp.concatenate(part, axis=1).astype(BF)
        turned = []
        for k in range(modes):
            turned.append(-width[k] * part[2 * k] - level[k] * part[2 * k + 1])
            turned.append(level[k] * part[2 * k] - width[k] * part[2 * k + 1])

        def summed(values):
            out = []
            for p in range(2):
                for l in range(leads):
                    total = hot[0][l] * values[p]
                    for k in range(1, modes):
                        total = total + hot[k][l] * values[2 * k + p]
                    out.append(total)
            return jnp.concatenate(out, axis=1)

        l_sum = summed(part)
        held[rows, :] = l_sum.astype(BF)
        f = jnp.concatenate([f_re[rows, :], f_im[rows, :]], axis=1)
        for i, a in enumerate((l_sum, summed(turned), f)):
            a = a.reshape(2, 2, 8, 2 * q).astype(BF)
            for c in range(2):
                pay[c, t // 4, pl.ds(2 * lax.rem(t, 4), 2), pl.ds(8 * i, 8), :] = a[:, c]
        return carry

    lax.fori_loop(0, pi.shape[0] // 32, chunk, 0)
    n_re = dot(held[:, :q], g_row[...], 0, 0)
    n_im = -dot(held[:, q:], g_row[...], 0, 0)
    n = jnp.concatenate([n_re, n_im], axis=1).astype(BF)
    pay[0, :, :, 24:32, :] = n.reshape(NY, NZ, 8, 2 * q)
    lane = lax.broadcasted_iota(jnp.int32, (8, 2 * q), 1)
    scal = jnp.zeros((8, 2 * q), F32)
    for i, weights in enumerate((re, im, [re[k] * occ[k] for k in range(modes)], [im[k] * occ[k] for k in range(modes)])):
        for l in range(leads):
            scal = jnp.where(lane == i * leads + l, sum(weights[k] * hot[k][l] for k in range(modes)), scal)
    pay[1, :, :, 24:32, :] = jnp.broadcast_to(scal.astype(BF), (NY, NZ, 8, 2 * q))


def local_sums(lead, coef, aux, f_re, f_im, g_row):
    rows, q = g_row.shape
    vm = pl.BlockSpec(memory_space=pltpu.VMEM)
    sm = pl.BlockSpec(memory_space=pltpu.SMEM)
    return pl.pallas_call(
        sums_kernel,
        out_shape=[
            jax.ShapeDtypeStruct((rows, aux.size // rows), BF),
            jax.ShapeDtypeStruct((2, NY, NZ, 32, 2 * q), BF),
        ],
        in_specs=[sm, sm, vm, vm, vm, vm],
        out_specs=[vm, vm],
        scratch_shapes=[pltpu.VMEM((rows, 2 * q), BF)],
        compiler_params=pltpu.CompilerParams(vmem_limit_bytes=24 * 1024 * 1024),
        name="sums",
    )(lead, coef, aux, f_re, f_im, g_row)


def modes_kernel(lead, coef, aux, ham, ham2, pi, src, u, g, hg, out, hp, h2p):
    k = pl.program_id(0)
    coupled = aux.shape[1]
    rows = ham.shape[0]
    modes = aux.shape[0] // (2 * rows)
    q = g.shape[1]
    hp[...] = dot(ham[...], pi[...])
    h2p[...] = dot(ham2[...], pi[...])
    level, width, wr, wi, occ = (coef[i, k] for i in range(5))
    first = pl.multiple_of(lead[k] * coupled, coupled)
    re, im = pl.ds(first, coupled), pl.ds(pl.multiple_of(q + first, coupled), coupled)
    lr, li = -width, level
    ar, ai = 3 + 2 * H2 * lr, 2 * H2 * li
    cr = 3 * lr + 2 * H2 * (lr * lr - li * li)
    ci = 3 * li + 4 * H2 * lr * li
    er, ei = 4 * H2 * li, -3 - 4 * H2 * lr
    size = 64

    def chunk(t, carry):
        at = pl.ds(pl.multiple_of(size * t, size), size)
        gk, hgk = occ * g[at, re].astype(F32), 2 * H2 * occ * hg[at, re]
        br, bi = src[at, re] - gk, src[at, im] - gk
        tr = ar * br - ai * bi + u[at, re] - hgk
        ti = ar * bi + ai * br + u[at, im] + hgk
        start = pl.multiple_of(size * t * 2 * modes, size) + 2 * k
        at_re = pl.ds(start, size, stride=2 * modes)
        at_im = pl.ds(start + 1, size, stride=2 * modes)
        pr, pim = aux[at_re, :], aux[at_im, :]
        hr, hi = hp[at, :coupled], hp[at, coupled:]
        out[at_re, :] = cr * pr - ci * pim + er * hr - ei * hi - 2 * H2 * h2p[at, :coupled] + wr * tr - wi * ti
        out[at_im, :] = cr * pim + ci * pr + er * hi + ei * hr - 2 * H2 * h2p[at, coupled:] + wr * ti + wi * tr
        return carry

    lax.fori_loop(0, rows // size, chunk, 0)


def advance_modes(lead, coef, aux, ham, ham2, pi, src, u, g, hg):
    rows, n = ham.shape
    coupled = aux.shape[1]
    modes = aux.shape[0] // (2 * rows)
    sm = pl.BlockSpec(memory_space=pltpu.SMEM)

    def whole(a):
        return pl.BlockSpec(a.shape, lambda k: (0,) * a.ndim)

    return pl.pallas_call(
        modes_kernel,
        grid=(modes,),
        out_shape=jax.ShapeDtypeStruct(aux.shape, F32),
        in_specs=[sm, sm, whole(aux), whole(ham), whole(ham2), pl.BlockSpec((n, 2 * coupled), lambda k: (0, k))]
        + [whole(a) for a in (src, u, g, hg)],
        out_specs=whole(aux),
        scratch_shapes=[pltpu.VMEM((rows, 2 * coupled), F32)] * 2,
        compiler_params=pltpu.CompilerParams(vmem_limit_bytes=40 * 1024 * 1024),
        cost_estimate=pl.CostEstimate(flops=4 * rows * n * 2 * coupled * modes, bytes_accessed=16 * 1024 * 1024, transcendentals=0),
        name="modes",
    )(lead, coef, aux, ham, ham2, pi, src, u, g, hg)


def by_lead(x, gamma):
    leads, coupled = gamma.shape[:2]
    return jnp.concatenate(
        [dot(x[:, l * coupled : (l + 1) * coupled], gamma[l]) for l in range(leads)], axis=1
    )


def shards(density, auxiliary, hamiltonian, coupling, lead_index, mode_level, mode_width, residue, occupation, lead_gamma):
    rows, cols = density.shape[1:]
    n = hamiltonian.shape[1]
    leads, coupled = coupling.shape
    q = leads * coupled
    modes = auxiliary.shape[1]
    n_mode = lax.axis_size("mode")
    n_row = lax.axis_size("row")
    x_pos, m_pos = lax.axis_index("row"), lax.axis_index("mode")
    row_start, col_start = x_pos * rows, m_pos * cols
    flat = coupling.reshape(-1)

    e_full = (jnp.arange(n, dtype=jnp.int32)[:, None] == flat[None, :]).astype(BF)
    e_row = (row_start + jnp.arange(rows, dtype=jnp.int32)[:, None] == flat[None, :]).astype(BF)
    e_col = (col_start + jnp.arange(cols, dtype=jnp.int32)[:, None] == flat[None, :]).astype(BF)
    g_row = by_lead(e_row, lead_gamma).astype(BF)
    g_col = by_lead(e_col, lead_gamma).astype(BF)

    rho_t = jnp.swapaxes(density, 1, 2).astype(BF).reshape(2 * cols, rows)
    ham_ct = jnp.swapaxes(lax.dynamic_slice_in_dim(hamiltonian, col_start, cols, 1), 0, 1)

    first = over_row(jnp.concatenate([ham_ct, rho_t], axis=0), 2)
    ham_c = first[:cols]
    applied = dot(first, hamiltonian, 1, 1)
    ham2_ct = applied[:cols].astype(BF)
    hrho_t = applied[cols:]
    he_row = dot(hamiltonian, e_full)
    hg_row = by_lead(he_row.astype(BF), lead_gamma)
    he_col = dot(ham_c, e_full).astype(BF)
    hg_col = by_lead(he_col, lead_gamma)

    hrho_b = hrho_t.astype(BF)
    f_re = dot(jnp.concatenate([hrho_b[cols:], rho_t[cols:]], 0), jnp.concatenate([2 * g_col, -hg_col.astype(BF)], 0), 0, 0)
    f_im = dot(jnp.concatenate([hrho_b[:cols], rho_t[:cols]], 0), jnp.concatenate([-2 * g_col, hg_col.astype(BF)], 0), 0, 0)
    coef = jnp.stack([mode_level, mode_width, residue[:, 0], residue[:, 1], occupation])
    aux = auxiliary.reshape(-1, coupled)
    pi_b, payload = local_sums(lead_index, coef, aux, f_re, f_im, g_row)
    piece = rows // n_mode
    pi_all, panel, whole = exchange(pi_b, jnp.concatenate([rho_t, ham2_ct], 0), payload)
    pi_all = pi_all.reshape(n, -1)
    panel = panel.reshape(n_mode, 3, cols, rows)
    ham2_all = panel[:, 2].reshape(n, rows)
    panel = [panel[:, p].reshape(n, rows) for p in range(2)]
    whole = whole.reshape(n_mode, 32, 2 * q)
    l1_b = whole[:, :piece].reshape(rows, 2 * q)
    m1 = whole[:, piece : 2 * piece].reshape(rows, 2 * q).astype(F32)
    f_all = whole[:, 2 * piece : 3 * piece].reshape(rows, 2 * q).astype(F32)
    n_all = whole[0::2, 3 * piece :].reshape(q, 2 * q)
    scal = whole[1, 3 * piece].astype(F32)
    w_sum, v_sum = scal[: 2 * leads], scal[2 * leads : 4 * leads]

    grow_full = by_lead(e_full, lead_gamma).astype(BF)
    src = jnp.concatenate([dot(panel[p], grow_full, 0, 0) for p in range(2)], axis=1)
    w_q = jnp.repeat(w_sum, coupled)
    v_q = jnp.repeat(v_sum, coupled)
    s_re, s_im = src[:, :q], src[:, q:]
    g_row_f = g_row.astype(F32)
    drive = jnp.concatenate(
        [w_q[:q] * s_re - w_q[q:] * s_im - (v_q[:q] - v_q[q:]) * g_row_f, w_q[:q] * s_im + w_q[q:] * s_re - (v_q[:q] + v_q[q:]) * g_row_f], axis=1
    )
    x_row = (3.0 * l1_b.astype(F32) + 2 * H2 * (m1 + drive)).astype(BF)
    p1 = jnp.concatenate([dot(e_col, l1_b[:, p * q : (p + 1) * q], 1, 1) for p in range(2)], 0)
    xe = jnp.concatenate([dot(e_col, x_row[:, p * q : (p + 1) * q], 1, 1) for p in range(2)], 0)
    rhoh_t = jnp.concatenate([dot(ham_c, panel[p]) for p in range(2)], 0)
    y = hrho_t - 2.0 * rhoh_t + 2.0 * jnp.concatenate([-p1[cols:], p1[:cols]], 0)
    z = dot(lax.dynamic_slice_in_dim(ham_c, row_start, rows, 1), l1_b)
    owner = col_start // rows
    own_l = lax.dynamic_slice_in_dim(l1_b, col_start - owner * rows, cols, 0)
    own_x = lax.dynamic_slice_in_dim(x_row, col_start - owner * rows, cols, 0)
    mask = (x_pos == owner).astype(BF)
    second = over_row(jnp.concatenate([y.astype(BF), ham2_ct, z.astype(BF), own_l * mask, own_x * mask], 0), 3)
    third = second[3 * cols :].astype(F32)
    third = sum(third[:, i * rows : (i + 1) * rows] for i in range(n_row))
    z, l_c, x_c = third[:cols], third[cols : 2 * cols], third[2 * cols :]
    hy = dot(second[: 2 * cols], hamiltonian, 1, 1)
    ham2_c = second[2 * cols : 3 * cols]
    rhoh2_t = jnp.concatenate([dot(ham2_c, panel[p]) for p in range(2)], 0)
    b_re = x_c[:, :q] + 4 * H2 * z[:, q:]
    b_im = -x_c[:, q:] + 4 * H2 * z[:, :q]
    back_re = dot(b_re.astype(BF), e_row, 1, 1)
    back_im = dot(b_im.astype(BF), e_row, 1, 1)
    l_cb = l_c.astype(BF)
    he_row_b = he_row.astype(BF)
    c1_re, c1_im = dot(l_cb[:, :q], he_row_b, 1, 1), -dot(l_cb[:, q:], he_row_b, 1, 1)
    c2_re, c2_im = dot(he_col, l1_b[:, :q], 1, 1), dot(he_col, l1_b[:, q:], 1, 1)
    d_re, d_im = c1_re - c2_re, c1_im - c2_im
    comm = hrho_t - rhoh_t
    base = -2 * H2 * (hy + rhoh2_t) + xe
    out_re = 3.0 * comm[cols:] + base[:cols] + back_re + 2 * H2 * d_im
    out_im = -3.0 * comm[:cols] + base[cols:] + back_im - 2 * H2 * d_re
    density_rate = jnp.swapaxes(jnp.stack([out_re, out_im]), 1, 2)

    lg = jnp.concatenate([by_lead(l1_b[:, p * q : (p + 1) * q], lead_gamma) for p in range(2)], 1)
    u = 2 * H2 * (f_all + lg + dot(e_row, n_all))
    auxiliary_rate = advance_modes(
        lead_index, coef, aux, hamiltonian, jnp.swapaxes(ham2_all, 0, 1), pi_all, src, u, g_row, hg_row
    ).reshape(auxiliary.shape)
    return density_rate, auxiliary_rate


def solution(mesh):
    in_specs = (
        P(None, "row", "mode"),
        P("row", "mode", None, None),
        P("row", None),
        P(),
        P("mode"),
        P("mode"),
        P("mode"),
        P("mode", None),
        P("mode"),
        P(),
    )
    out_specs = (P(None, "row", "mode"), P("row", "mode", None, None))
    return jax.shard_map(shards, mesh=mesh, in_specs=in_specs, out_specs=out_specs, check_vma=False)
```

```python
import jax
import jax.numpy as jnp
from jax import lax
from jax.experimental import pallas as pl
from jax.experimental.pallas import tpu as pltpu
from jax.sharding import PartitionSpec as P

H2 = 0.05
F32 = jnp.float32
BF = jnp.bfloat16


def dot(a, b, ca=1, cb=0):
    return lax.dot_general(a, b, (((ca,), (cb,)), ((), ())), preferred_element_type=F32)


MESH = pl.DeviceIdType.MESH
NY, NZ = 4, 8


class Net:
    def __init__(self, send, recv):
        self.send, self.recv, self.used, self.sent = send, recv, 0, []
        m = lax.axis_index("mode")
        self.x = lax.axis_index("row")
        self.c, self.z, self.y = lax.rem(m, 2), lax.rem(m // 2, NZ), m // (2 * NZ)

    def dev(self, y=None, z=None, c=None, x=None):
        y = self.y if y is None else y
        z = self.z if z is None else z
        c = self.c if c is None else c
        return {"mode": (y * NZ + z) * 2 + c, "row": self.x if x is None else x}

    def at(self, name, d):
        size = {"x": 4, "y": NY, "z": NZ}[name]
        return lax.rem(getattr(self, name) + (d % size), size)

    def slot(self):
        self.used += 1
        return self.used - 1

    def start(self, src, dst, to, slot):
        copy = pltpu.make_async_remote_copy(
            src_ref=src, dst_ref=dst, send_sem=self.send.at[slot], recv_sem=self.recv.at[slot], device_id=to, device_id_type=MESH
        )
        copy.start()
        self.sent.append(copy)

    def arrive(self, ref, slot):
        pltpu.make_async_remote_copy(
            src_ref=ref, dst_ref=ref, send_sem=self.send.at[slot], recv_sem=self.recv.at[slot],
            device_id=self.dev(c=1 - self.c), device_id_type=MESH,
        ).wait_recv()

    def finish(self):
        for copy in self.sent:
            copy.wait_send()

    def greet(self, peers):
        barrier = pltpu.get_barrier_semaphore()
        for peer in peers:
            pl.semaphore_signal(barrier, inc=1, device_id=peer, device_id_type=MESH)
        pl.semaphore_wait(barrier, len(peers))


def ring(net, name, part, share, t, step):
    size = {"x": 4, "y": NY, "z": NZ}[name]
    far = size // 2
    slots = {(d, s): net.slot() for s in range(1, far + 1) for d in (1, -1)}
    at = lambda d: net.at(name, d)
    for d in (1, -1):
        net.start(part(at(0), None), part(at(0), None), net.dev(**{name: at(d)}), slots[d, 1])
    share(at(0))
    for s in range(1, far + 1):
        yield t + s * step
        for d in (1, -1):
            half = None if s < far else (d + 1) // 2
            net.arrive(part(at(-d * s), half), slots[d, s])
            if s < far:
                half = None if s + 1 < far else (d + 1) // 2
                net.start(part(at(-d * s), half), part(at(-d * s), half), net.dev(**{name: at(d)}), slots[d, s + 1])
        if s < far:
            share(at(s))
            share(at(-s))
        else:
            share(at(far))


def gather_plane(net, buf, t, unit):
    rows, lanes = buf.shape[-2:]
    lane = {None: pl.ds(0, lanes), 0: pl.ds(0, lanes // 2), 1: pl.ds(lanes // 2, lanes // 2)}
    low, high = pl.ds(0, rows // 2), pl.ds(rows // 2, rows // 2)
    c = net.c
    waits = []

    def share_of(ref_of):
        def share(pos):
            slot = net.slot()
            mine, theirs = ref_of(pos, c), ref_of(pos, 1 - c)
            net.start(mine, mine, net.dev(c=1 - c), slot)
            waits.append((theirs, slot))
        return share

    def nothing(pos):
        pass

    def first():
        yield from ring(net, "y", lambda p, h: buf.at[:, p, net.z, c, low, lane[h]], nothing, t, 2.0 + unit)
        yield from ring(
            net, "z", lambda p, h: buf.at[:, :, p, c, low, lane[h]],
            share_of(lambda p, cc: buf.at[:, :, p, cc, low, lane[None]]), t + 5.0 + 2 * unit, 2.0 + 4 * unit,
        )

    def second():
        yield from ring(net, "z", lambda p, h: buf.at[:, net.y, p, c, high, lane[h]], nothing, t, 2.0 + unit)
        yield from ring(
            net, "y", lambda p, h: buf.at[:, p, :, c, high, lane[h]],
            share_of(lambda p, cc: buf.at[:, p, :, cc, high, lane[None]]), t + 9.0 + 4 * unit, 2.0 + 8 * unit,
        )

    yield from merge([first(), second()])
    yield t + 12.0 + 30 * unit
    for ref, slot in waits:
        net.arrive(ref, slot)


def gather_small(net, whole, rows, lanes, t, unit):
    c = net.c
    slots = [net.slot() for _ in range(NZ - 1)]
    mine = whole.at[net.y, net.z, c, rows, lanes]
    for d in (4, 3, 5, 2, 6, 1, 7):
        net.start(mine, mine, net.dev(z=net.at("z", d)), slots[d - 1])
    yield t + 4.0 + 10 * unit
    for d in (1, 7, 2, 6, 3, 5, 4):
        net.arrive(whole.at[net.y, net.at("z", -d), c, rows, lanes], slots[d - 1])
    cuts = {None: pl.ds(0, NZ), 0: pl.ds(0, NZ // 2), 1: pl.ds(NZ // 2, NZ // 2)}
    waits = []

    def share(pos):
        slot = net.slot()
        ref = whole.at[pos, :, c, rows, lanes]
        net.start(ref, ref, net.dev(c=1 - c), slot)
        waits.append((whole.at[pos, :, 1 - c, rows, lanes], slot))

    yield from ring(net, "y", lambda p, h: whole.at[p, cuts[h], c, rows, lanes], share, t + 4.0 + 10 * unit, 2.0 + 6 * unit)
    yield t + 10.0 + 24 * unit
    for ref, slot in waits:
        net.arrive(ref, slot)


def merge(threads):
    live = []
    for thread in threads:
        when = next(thread, None)
        if when is not None:
            live.append([when, len(live), thread])
    while live:
        live.sort(key=lambda item: (item[0], item[1]))
        yield live[0][0]
        when = next(live[0][2], None)
        if when is None:
            live.pop(0)
        else:
            live[0][0] = when


def reduce_plane(net, chain, pay, whole, tails, scal, xs, pair, acc, got1, got2, gotz, t):
    c, y, z = net.c, net.y, net.z
    width = got2.shape[-1]
    ln = pl.ds(chain * width, width)
    slot = net.slot()
    net.start(pay.at[1 - c, :, :, :, ln], pair.at[:, :, :, ln], net.dev(c=1 - c), slot)
    yield t + 2.0
    net.arrive(pair.at[:, :, :, ln], slot)

    def add_pair(i, carry):
        acc[i, :, :, ln] = (pay[c, i, :, :, ln].astype(F32) + pair[i, :, :, ln].astype(F32)).astype(BF)
        return carry

    lax.fori_loop(0, NY, add_pair, 0)
    near, over = y + 1 - 2 * lax.rem(y, 2), NY - 1 - y
    half = NZ // 2
    colors = []
    for color, (f, s) in enumerate(((near, over), (over, near))):
        s_of_f = lax.rem(y + 2, NY)
        zs = pl.ds(color * half, half)
        slots = [net.slot() for _ in range(3)]
        net.start(acc.at[s_of_f, zs, :, ln], got1.at[chain, color, 1], net.dev(y=f), slots[1])
        net.start(acc.at[f, zs, :, ln], got1.at[chain, color, 0], net.dev(y=f), slots[0])
        colors.append((f, s, zs, slots))
    yield t + 5.5
    for color, (f, s, zs, slots) in enumerate(colors):
        net.arrive(got1.at[chain, color, 1], slots[1])
        acc[s, zs, :, ln] = (acc[s, zs, :, ln].astype(F32) + got1[chain, color, 1].astype(F32)).astype(BF)
        net.start(acc.at[s, zs, :, ln], got2.at[chain, color], net.dev(y=s), slots[2])
    yield t + 9.5
    for color, (f, s, zs, slots) in enumerate(colors):
        net.arrive(got1.at[chain, color, 0], slots[0])
        net.arrive(got2.at[chain, color], slots[2])
        total = acc[y, zs, :, ln].astype(F32) + got1[chain, color, 0].astype(F32) + got2[chain, color].astype(F32)
        acc[y, zs, :, ln] = total.astype(BF)
    zslots = [net.slot() for _ in range(NZ - 1)]
    for d in (4, 3, 5, 2, 6, 1, 7):
        net.start(acc.at[y, net.at("z", d), :, ln], gotz.at[chain, d - 1], net.dev(z=net.at("z", d)), zslots[d - 1])
    yield t + 16.0
    total = acc[y, z, :, ln].astype(F32)
    for d in range(1, NZ):
        net.arrive(gotz.at[chain, d - 1], zslots[d - 1])
        total = total + gotz[chain, d - 1].astype(F32)
    whole[y, z, c, :, ln] = total[:16].astype(BF)
    tails[pl.ds(0, 8), ln] = total[16:24]
    xs[0, :, ln] = total[24:]
    slots = [net.slot() for _ in range(4)]
    mine = xs.at[0, :, ln]
    net.start(mine, xs.at[4, :, ln], net.dev(c=1 - c), slots[0])
    for d in (1, 2, 3):
        net.start(mine, xs.at[d, :, ln], net.dev(x=net.at("x", d)), slots[d])

    def small_ends():
        yield t + 34.0
        for d, slot in zip((4, 1, 2, 3), slots):
            net.arrive(xs.at[d, :, ln], slot)
        tails[pl.ds(8, 8), ln] = xs[0, :, ln] + xs[1, :, ln] + xs[2, :, ln] + xs[3, :, ln]
        scal[:, ln] = jnp.where(jnp.full((8, width), c) == 1, xs[0, :, ln], xs[4, :, ln])

    yield from merge([gather_small(net, whole, pl.ds(0, 16), ln, t + 16.0, 0.2), small_ends()])


def gather_rows(net, pall):
    rows = pall.shape[1] // 2
    halves = (pl.ds(0, rows), pl.ds(rows, rows))
    x = net.x
    slots = {(d, i): net.slot() for d in (0, 1) for i in range(3)}
    for i in (0, 1):
        for d, way in ((0, 1), (1, -1)):
            ref = pall.at[x, halves[i if d == 0 else 1 - i]]
            net.start(ref, ref, net.dev(x=net.at("x", way)), slots[d, i])
    yield 16.0
    for d, way in ((0, 1), (1, -1)):
        ref = pall.at[net.at("x", -way), halves[d]]
        net.arrive(ref, slots[d, 0])
        net.start(ref, ref, net.dev(x=net.at("x", way)), slots[d, 2])
    yield 40.0
    for d, way in ((0, 1), (1, -1)):
        net.arrive(pall.at[net.at("x", -way), halves[1 - d]], slots[d, 1])
        net.arrive(pall.at[net.at("x", -2), halves[d]], slots[d, 2])


def spread_rows(net, src, place):
    slots = [net.slot() for _ in range(3)]
    for d in (2, 1, 3):
        net.start(src, place(net.x), net.dev(x=net.at("x", d)), slots[d - 1])

    def arrived():
        for d in (1, 3, 2):
            net.arrive(place(net.at("x", -d)), slots[d - 1])

    return arrived


def lanes_of(ref, x, lanes):
    at = pl.ds(pl.multiple_of(x * lanes, lanes), lanes)
    return ref.at[(slice(None),) * (len(ref.shape) - 1) + (at,)]


def front_kernel(
    lead, coef, aux, blk, ham, flat, gamma,
    first, hrho, ham2x, pall, panel, ham2, whole, tails, scal, grow, he_row, hg_row, he_col,
    picks, xs, own2, pay, held, pair, acc, got1, got2, gotz, send, recv,
):
    net = Net(send, recv)
    c, y, z, x = net.c, net.y, net.z, net.x
    peers = [net.dev(x=net.at("x", d)) for d in (1, 2, 3)]
    peers += [net.dev(y=net.at("y", d)) for d in (1, 3)]
    peers += [net.dev(z=net.at("z", d)) for d in range(1, NZ)]
    peers += [net.dev(c=1 - c)]
    net.greet(peers)
    cols, rows = blk.shape[1:]
    arrived = spread_rows(net, blk, lambda at: lanes_of(first, at, rows))
    panel[:, y, z, c] = blk[1:]
    lanes_of(first, x, rows)[...] = blk[...]

    def pick(i, carry):
        at = pl.ds(pl.multiple_of(256 * i, 256), 256)
        here = 256 * i + lax.broadcasted_iota(jnp.int32, (256, flat.shape[1]), 0)
        e = jnp.where(here == flat[...], 1.0, 0.0).astype(BF)
        picks[at, :] = e
        grow[at, :] = by_lead(e, gamma).astype(BF)
        return carry

    def work():
        lax.fori_loop(0, picks.shape[0] // 256, pick, 0)
        g_row = grow[pl.ds(pl.multiple_of(x * rows, rows), rows), :]
        sums(lead, coef, aux, g_row, pall, x, pay, held)
        rows_thread = gather_rows(net, pall)
        start = next(rows_thread)
        yield from merge([more(), resumed(rows_thread, start)])

    def more():
        yield 9.0
        arrived()
        applied = dot(first[...].reshape(3 * cols, -1), ham[...], 1, 1)
        own2[...] = applied[:cols].astype(BF)
        ham2[0, y, z, c] = own2[...]
        hrho[...] = applied[cols:]
        hg = dot(first[0], grow[...]).astype(BF)
        lhs = jnp.concatenate([applied[cols:].astype(BF), blk[1:].reshape(2 * cols, rows)], axis=0)
        me = (y * NZ + z) * 2 + c
        g2 = 2 * grow[pl.ds(pl.multiple_of(me * cols, cols), cols), :]
        for i, (sign, p) in enumerate(((1, 1), (-1, 0))):
            left = jnp.concatenate([lhs[p * cols : (p + 1) * cols], lhs[(2 + p) * cols : (3 + p) * cols]], axis=0)
            f = dot(left, sign * jnp.concatenate([g2, -hg], axis=0), 0, 0)
            q = f.shape[1]
            f = f.astype(BF).reshape(NY, NZ, 2, 8, q)
            for cc in range(2):
                pay[cc, :, :, 16:24, i * q : (i + 1) * q] = f[:, :, cc]
        chains = [reduce_plane(net, i, pay, whole, tails, scal, xs, pair, acc, got1, got2, gotz, 10.0 + 3.0 * i) for i in range(2)]
        spread = spread_ham2()
        yield from merge([*chains, gather_plane(net, ham2, 11.0, 0.4), spread, spare()])

    def spare():
        yield 13.8
        he_row[...] = dot(ham[...], picks[...]).astype(BF)
        hg_row[...] = dot(ham[...], grow[...])
        he_col[...] = dot(first[0], picks[...]).astype(BF)

    def spread_ham2():
        here = spread_rows(net, own2, lambda at: lanes_of(ham2x, at, rows))
        lanes_of(ham2x, x, rows)[...] = own2[...]
        yield 41.0
        here()

    for _ in merge([gather_plane(net, panel, 1.0, 0.75), work()]):
        pass
    net.finish()


def resumed(thread, start):
    yield start
    yield from thread


def front(lead, coef, aux, blk, ham, flat, gamma):
    cols, lanes = blk.shape[1:]
    half = lanes // 2
    n = ham.shape[1]
    vm = pl.BlockSpec(memory_space=pltpu.VMEM)
    sm = pl.BlockSpec(memory_space=pltpu.SMEM)
    sems = 192
    return pl.pallas_call(
        front_kernel,
        out_shape=[
            jax.ShapeDtypeStruct((3, cols, n), BF),
            jax.ShapeDtypeStruct((2 * cols, lanes), F32),
            jax.ShapeDtypeStruct((cols, n), BF),
            jax.ShapeDtypeStruct((4, lanes, aux.size // lanes), BF),
            jax.ShapeDtypeStruct((2, NY, NZ, 2, cols, lanes), BF),
            jax.ShapeDtypeStruct((1, NY, NZ, 2, cols, lanes), BF),
            jax.ShapeDtypeStruct((NY, NZ, 2, 16, lanes), BF),
            jax.ShapeDtypeStruct((16, lanes), F32),
            jax.ShapeDtypeStruct((8, lanes), F32),
            jax.ShapeDtypeStruct((n, flat.shape[1]), BF),
            jax.ShapeDtypeStruct((lanes, flat.shape[1]), BF),
            jax.ShapeDtypeStruct((lanes, flat.shape[1]), F32),
            jax.ShapeDtypeStruct((cols, flat.shape[1]), BF),
        ],
        in_specs=[sm, sm] + [vm] * 5,
        out_specs=[vm] * 13,
        scratch_shapes=[
            pltpu.VMEM((n, flat.shape[1]), BF),
            pltpu.VMEM((5, 8, lanes), F32),
            pltpu.VMEM((cols, lanes), BF),
            pltpu.VMEM((2, NY, NZ, 32, lanes), BF),
            pltpu.VMEM((lanes, lanes), BF),
            pltpu.VMEM((NY, NZ, 32, lanes), BF),
            pltpu.VMEM((NY, NZ, 32, lanes), BF),
            pltpu.VMEM((2, 2, 2, NZ // 2, 32, half), BF),
            pltpu.VMEM((2, 2, NZ // 2, 32, half), BF),
            pltpu.VMEM((2, NZ - 1, 32, half), BF),
            pltpu.SemaphoreType.DMA((sems,)),
            pltpu.SemaphoreType.DMA((sems,)),
        ],
        compiler_params=pltpu.CompilerParams(collective_id=1, has_side_effects=True, vmem_limit_bytes=30 * 1024 * 1024),
        cost_estimate=pl.CostEstimate(flops=10**11, bytes_accessed=2**24, transcendentals=0),
        name="front",
    )(lead, coef, aux, blk, ham, flat, gamma)


def back_kernel(blk, tails, out, n_all, send, recv):
    net = Net(send, recv)
    peers = [net.dev(x=net.at("x", d)) for d in (1, 2, 3)]
    peers += [net.dev(y=net.at("y", d)) for d in (1, 3)]
    peers += [net.dev(z=net.at("z", d)) for d in range(1, NZ)]
    peers += [net.dev(c=1 - net.c)]
    net.greet(peers)
    lanes = blk.shape[1]
    lanes_of(out, net.x, lanes)[...] = blk[...]
    n_all[net.y, net.z, net.c] = tails[...].astype(BF)
    half = lanes // 2
    cuts = {None: (0, lanes), 0: (0, half), 1: (half, half)}

    def part(at, h):
        first, width = cuts[h]
        return out.at[:, pl.ds(pl.multiple_of(at * lanes + first, half), width)]

    for _ in merge([ring(net, "x", part, lambda at: None, 0.0, 4.0), gather_small(net, n_all, pl.ds(0, 16), pl.ds(0, lanes), 0.0, 0.2)]):
        pass
    net.finish()


def back(blk, tails):
    lanes = blk.shape[1]
    vm = pl.BlockSpec(memory_space=pltpu.VMEM)
    return pl.pallas_call(
        back_kernel,
        out_shape=[
            jax.ShapeDtypeStruct((blk.shape[0], 4 * lanes), BF),
            jax.ShapeDtypeStruct((NY, NZ, 2, 16, lanes), BF),
        ],
        in_specs=[vm] * 2,
        out_specs=[vm] * 2,
        scratch_shapes=[
            pltpu.SemaphoreType.DMA((32,)),
            pltpu.SemaphoreType.DMA((32,)),
        ],
        compiler_params=pltpu.CompilerParams(collective_id=2, has_side_effects=True, vmem_limit_bytes=8 * 1024 * 1024),
        cost_estimate=pl.CostEstimate(flops=3 * 10**10, bytes_accessed=2**20, transcendentals=0),
        name="back",
    )(blk, tails)


def sums(lead, coef, aux, g_row, pall, x, pay, held):
    q = g_row.shape[1]
    coupled = aux.shape[1]
    modes = aux.shape[0] // (2 * held.shape[0])
    leads = q // coupled
    hot = [[jnp.where(lead[k] == l, 1.0, 0.0) for l in range(leads)] for k in range(modes)]
    level, width, re, im, occ = ([coef[i, k] for k in range(modes)] for i in range(5))

    def chunk(t, carry):
        rows = pl.ds(pl.multiple_of(32 * t, 32), 32)
        part = [aux[pl.ds(pl.multiple_of(32 * t * 2 * modes, 32) + i, 32, stride=2 * modes), :] for i in range(2 * modes)]
        pall[x, rows, :] = jnp.concatenate(part, axis=1).astype(BF)
        turned = []
        for k in range(modes):
            turned.append(-width[k] * part[2 * k] - level[k] * part[2 * k + 1])
            turned.append(level[k] * part[2 * k] - width[k] * part[2 * k + 1])

        def summed(values):
            out = []
            for p in range(2):
                for l in range(leads):
                    total = hot[0][l] * values[p]
                    for k in range(1, modes):
                        total = total + hot[k][l] * values[2 * k + p]
                    out.append(total)
            return jnp.concatenate(out, axis=1)

        l_sum = summed(part)
        held[rows, :] = l_sum.astype(BF)
        for i, a in enumerate((l_sum, summed(turned))):
            a = a.reshape(2, 2, 8, 2 * q).astype(BF)
            for c in range(2):
                pay[c, t // 4, pl.ds(2 * lax.rem(t, 4), 2), pl.ds(8 * i, 8), :] = a[:, c]
        return carry

    lax.fori_loop(0, held.shape[0] // 32, chunk, 0)
    n_re = dot(held[:, :q], g_row, 0, 0)
    n_im = -dot(held[:, q:], g_row, 0, 0)
    n = jnp.concatenate([n_re, n_im], axis=1).astype(BF)
    pay[0, :, :, 24:32, :] = n.reshape(NY, NZ, 8, 2 * q)
    lane = lax.broadcasted_iota(jnp.int32, (8, 2 * q), 1)
    scal = jnp.zeros((8, 2 * q), F32)
    for i, weights in enumerate((re, im, [re[k] * occ[k] for k in range(modes)], [im[k] * occ[k] for k in range(modes)])):
        for l in range(leads):
            scal = jnp.where(lane == i * leads + l, sum(weights[k] * hot[k][l] for k in range(modes)), scal)
    pay[1, :, :, 24:32, :] = jnp.broadcast_to(scal.astype(BF), (NY, NZ, 8, 2 * q))


def modes_kernel(lead, coef, aux, ham, ham2, pi, src, u, g, hg, out, hp, h2p, turned):
    k = pl.program_id(0)

    @pl.when(k == 0)
    def _():
        for i in range(0, ham2.shape[0], 512):
            turned[:, i : i + 512] = ham2[i : i + 512, :].T

    coupled = aux.shape[1]
    rows = ham.shape[0]
    modes = aux.shape[0] // (2 * rows)
    q = g.shape[1]
    hp[...] = dot(ham[...], pi[...])
    h2p[...] = dot(turned[...], pi[...])
    level, width, wr, wi, occ = (coef[i, k] for i in range(5))
    first = pl.multiple_of(lead[k] * coupled, coupled)
    re, im = pl.ds(first, coupled), pl.ds(pl.multiple_of(q + first, coupled), coupled)
    lr, li = -width, level
    ar, ai = 3 + 2 * H2 * lr, 2 * H2 * li
    cr = 3 * lr + 2 * H2 * (lr * lr - li * li)
    ci = 3 * li + 4 * H2 * lr * li
    er, ei = 4 * H2 * li, -3 - 4 * H2 * lr
    size = 64

    def chunk(t, carry):
        at = pl.ds(pl.multiple_of(size * t, size), size)
        gk, hgk = occ * g[at, re].astype(F32), 2 * H2 * occ * hg[at, re]
        br, bi = src[at, re] - gk, src[at, im] - gk
        tr = ar * br - ai * bi + u[at, re] - hgk
        ti = ar * bi + ai * br + u[at, im] + hgk
        start = pl.multiple_of(size * t * 2 * modes, size) + 2 * k
        at_re = pl.ds(start, size, stride=2 * modes)
        at_im = pl.ds(start + 1, size, stride=2 * modes)
        pr, pim = aux[at_re, :], aux[at_im, :]
        hr, hi = hp[at, :coupled], hp[at, coupled:]
        out[at_re, :] = cr * pr - ci * pim + er * hr - ei * hi - 2 * H2 * h2p[at, :coupled] + wr * tr - wi * ti
        out[at_im, :] = cr * pim + ci * pr + er * hi + ei * hr - 2 * H2 * h2p[at, coupled:] + wr * ti + wi * tr
        return carry

    lax.fori_loop(0, rows // size, chunk, 0)


def advance_modes(lead, coef, aux, ham, ham2, pi, src, u, g, hg):
    rows, n = ham.shape
    coupled = aux.shape[1]
    modes = aux.shape[0] // (2 * rows)
    sm = pl.BlockSpec(memory_space=pltpu.SMEM)

    def whole(a):
        return pl.BlockSpec(a.shape, lambda k: (0,) * a.ndim)

    return pl.pallas_call(
        modes_kernel,
        grid=(modes,),
        out_shape=jax.ShapeDtypeStruct(aux.shape, F32),
        in_specs=[sm, sm, whole(aux), whole(ham), whole(ham2), pl.BlockSpec((n, 2 * coupled), lambda k: (0, k))]
        + [whole(a) for a in (src, u, g, hg)],
        out_specs=whole(aux),
        scratch_shapes=[pltpu.VMEM((rows, 2 * coupled), F32)] * 2 + [pltpu.VMEM((rows, n), BF)],
        compiler_params=pltpu.CompilerParams(vmem_limit_bytes=28 * 1024 * 1024),
        cost_estimate=pl.CostEstimate(flops=4 * rows * n * 2 * coupled * modes, bytes_accessed=16 * 1024 * 1024, transcendentals=0),
        name="modes",
    )(lead, coef, aux, ham, ham2, pi, src, u, g, hg)


def by_lead(x, gamma):
    leads, coupled = gamma.shape[:2]
    return jnp.concatenate(
        [dot(x[:, l * coupled : (l + 1) * coupled], gamma[l]) for l in range(leads)], axis=1
    )


def shards(density, auxiliary, hamiltonian, coupling, lead_index, mode_level, mode_width, residue, occupation, lead_gamma):
    rows, cols = density.shape[1:]
    n = hamiltonian.shape[1]
    leads, coupled = coupling.shape
    q = leads * coupled
    modes = auxiliary.shape[1]
    n_mode = lax.axis_size("mode")
    n_row = lax.axis_size("row")
    x_pos, m_pos = lax.axis_index("row"), lax.axis_index("mode")
    row_start, col_start = x_pos * rows, m_pos * cols
    flat = coupling.reshape(-1)

    e_row = (row_start + jnp.arange(rows, dtype=jnp.int32)[:, None] == flat[None, :]).astype(BF)
    e_col = (col_start + jnp.arange(cols, dtype=jnp.int32)[:, None] == flat[None, :]).astype(BF)
    rho_t = jnp.swapaxes(density, 1, 2).astype(BF).reshape(2 * cols, rows)
    ham_ct = jnp.swapaxes(lax.dynamic_slice_in_dim(hamiltonian, col_start, cols, 1), 0, 1)

    coef = jnp.stack([mode_level, mode_width, residue[:, 0], residue[:, 1], occupation])
    aux = auxiliary.reshape(-1, coupled)
    blk = jnp.concatenate([ham_ct, rho_t], axis=0).reshape(3, cols, rows)
    first, hrho_t, ham2_c, pi_all, panel, ham2_all, whole, tails, scal, grow_full, he_row_b, hg_row, he_col = front(
        lead_index, coef, aux, blk, hamiltonian, flat[None], lead_gamma
    )
    g_row = lax.dynamic_slice_in_dim(grow_full, row_start, rows, 0)
    ham_c = first[0]
    piece = rows // n_mode
    pi_all = pi_all.reshape(n, -1)
    panel = panel.reshape(2, n, rows)
    ham2_all = ham2_all.reshape(n, rows)
    whole = whole.reshape(n_mode, 2 * piece, 2 * q)
    l1_b = whole[:, :piece].reshape(rows, 2 * q)
    m1 = whole[:, piece : 2 * piece].reshape(rows, 2 * q).astype(F32)
    scal = scal[0]
    w_sum, v_sum = scal[: 2 * leads], scal[2 * leads : 4 * leads]

    src = dot(panel, grow_full, 1, 0)
    src = jnp.concatenate([src[0], src[1]], axis=1)
    w_q = jnp.repeat(w_sum, coupled)
    v_q = jnp.repeat(v_sum, coupled)
    s_re, s_im = src[:, :q], src[:, q:]
    g_row_f = g_row.astype(F32)
    drive = jnp.concatenate(
        [w_q[:q] * s_re - w_q[q:] * s_im - (v_q[:q] - v_q[q:]) * g_row_f, w_q[:q] * s_im + w_q[q:] * s_re - (v_q[:q] + v_q[q:]) * g_row_f], axis=1
    )
    x_row = (3.0 * l1_b.astype(F32) + 2 * H2 * (m1 + drive)).astype(BF)
    p1 = jnp.concatenate([dot(e_col, l1_b[:, p * q : (p + 1) * q], 1, 1) for p in range(2)], 0)
    xe = jnp.concatenate([dot(e_col, x_row[:, p * q : (p + 1) * q], 1, 1) for p in range(2)], 0)
    rhoh_t = jnp.swapaxes(dot(jnp.concatenate([ham_c, ham2_c], 0), panel, 1, 1), 0, 1)
    rhoh_t, rhoh2_t = (rhoh_t[:, i * cols : (i + 1) * cols].reshape(2 * cols, rows) for i in range(2))
    y = hrho_t - 2.0 * rhoh_t + 2.0 * jnp.concatenate([-p1[cols:], p1[:cols]], 0)
    z = dot(lax.dynamic_slice_in_dim(ham_c, row_start, rows, 1), l1_b)
    owner = col_start // rows
    own_l = lax.dynamic_slice_in_dim(l1_b, col_start - owner * rows, cols, 0)
    own_x = lax.dynamic_slice_in_dim(x_row, col_start - owner * rows, cols, 0)
    mask = (x_pos == owner).astype(BF)
    second, n_all = back(jnp.concatenate([y.astype(BF), z.astype(BF), own_l * mask, own_x * mask], 0), tails)
    f_all = n_all[..., :8, :].reshape(rows, 2 * q).astype(F32)
    n_all = n_all[:, :, 0, 8:].reshape(q, 2 * q)
    third = second[2 * cols :].astype(F32)
    third = sum(third[:, i * rows : (i + 1) * rows] for i in range(n_row))
    z, l_c, x_c = third[:cols], third[cols : 2 * cols], third[2 * cols :]
    hy = dot(second[: 2 * cols], hamiltonian, 1, 1)
    b_re = x_c[:, :q] + 4 * H2 * z[:, q:]
    b_im = -x_c[:, q:] + 4 * H2 * z[:, :q]
    back_re = dot(b_re.astype(BF), e_row, 1, 1)
    back_im = dot(b_im.astype(BF), e_row, 1, 1)
    l_cb = l_c.astype(BF)
    c1_re, c1_im = dot(l_cb[:, :q], he_row_b, 1, 1), -dot(l_cb[:, q:], he_row_b, 1, 1)
    c2_re, c2_im = dot(he_col, l1_b[:, :q], 1, 1), dot(he_col, l1_b[:, q:], 1, 1)
    d_re, d_im = c1_re - c2_re, c1_im - c2_im
    comm = hrho_t - rhoh_t
    base = -2 * H2 * (hy + rhoh2_t) + xe
    out_re = 3.0 * comm[cols:] + base[:cols] + back_re + 2 * H2 * d_im
    out_im = -3.0 * comm[:cols] + base[cols:] + back_im - 2 * H2 * d_re
    density_rate = jnp.swapaxes(jnp.stack([out_re, out_im]), 1, 2)

    lg = jnp.concatenate([by_lead(l1_b[:, p * q : (p + 1) * q], lead_gamma) for p in range(2)], 1)
    u = 2 * H2 * (f_all + lg + dot(e_row, n_all))
    auxiliary_rate = advance_modes(
        lead_index, coef, aux, hamiltonian, ham2_all, pi_all, src, u, g_row, hg_row
    ).reshape(auxiliary.shape)
    return density_rate, auxiliary_rate


def solution(mesh):
    in_specs = (
        P(None, "row", "mode"),
        P("row", "mode", None, None),
        P("row", None),
        P(),
        P("mode"),
        P("mode"),
        P("mode"),
        P("mode", None),
        P("mode"),
        P(),
    )
    out_specs = (P(None, "row", "mode"), P("row", "mode", None, None))
    return jax.shard_map(shards, mesh=mesh, in_specs=in_specs, out_specs=out_specs, check_vma=False)
```

```python
import jax
import jax.numpy as jnp
from jax import lax
from jax.experimental import pallas as pl
from jax.experimental.pallas import tpu as pltpu
from jax.sharding import PartitionSpec as P

H2 = 0.05
F32 = jnp.float32
BF = jnp.bfloat16


def dot(a, b, ca=1, cb=0):
    return lax.dot_general(a, b, (((ca,), (cb,)), ((), ())), preferred_element_type=F32)


MESH = pl.DeviceIdType.MESH
NY, NZ = 4, 8


class Net:
    def __init__(self, send, recv):
        self.send, self.recv, self.used, self.sent = send, recv, 0, []
        m = lax.axis_index("mode")
        self.x = lax.axis_index("row")
        self.c, self.z, self.y = lax.rem(m, 2), lax.rem(m // 2, NZ), m // (2 * NZ)

    def dev(self, y=None, z=None, c=None, x=None):
        y = self.y if y is None else y
        z = self.z if z is None else z
        c = self.c if c is None else c
        return {"mode": (y * NZ + z) * 2 + c, "row": self.x if x is None else x}

    def at(self, name, d):
        size = {"x": 4, "y": NY, "z": NZ}[name]
        return lax.rem(getattr(self, name) + (d % size), size)

    def slot(self):
        self.used += 1
        return self.used - 1

    def start(self, src, dst, to, slot):
        copy = pltpu.make_async_remote_copy(
            src_ref=src, dst_ref=dst, send_sem=self.send.at[slot], recv_sem=self.recv.at[slot], device_id=to, device_id_type=MESH
        )
        copy.start()
        self.sent.append(copy)

    def arrive(self, ref, slot):
        pltpu.make_async_remote_copy(
            src_ref=ref, dst_ref=ref, send_sem=self.send.at[slot], recv_sem=self.recv.at[slot],
            device_id=self.dev(c=1 - self.c), device_id_type=MESH,
        ).wait_recv()

    def finish(self):
        for copy in self.sent:
            copy.wait_send()

    def greet(self, peers):
        barrier = pltpu.get_barrier_semaphore()
        for peer in peers:
            pl.semaphore_signal(barrier, inc=1, device_id=peer, device_id_type=MESH)
        pl.semaphore_wait(barrier, len(peers))


def ring(net, name, part, share, t, step):
    size = {"x": 4, "y": NY, "z": NZ}[name]
    far = size // 2
    slots = {(d, s): net.slot() for s in range(1, far + 1) for d in (1, -1)}
    at = lambda d: net.at(name, d)
    for d in (1, -1):
        net.start(part(at(0), None), part(at(0), None), net.dev(**{name: at(d)}), slots[d, 1])
    share(at(0))
    for s in range(1, far + 1):
        yield t + s * step
        for d in (1, -1):
            half = None if s < far else (d + 1) // 2
            net.arrive(part(at(-d * s), half), slots[d, s])
            if s < far:
                half = None if s + 1 < far else (d + 1) // 2
                net.start(part(at(-d * s), half), part(at(-d * s), half), net.dev(**{name: at(d)}), slots[d, s + 1])
        if s < far:
            share(at(s))
            share(at(-s))
        else:
            share(at(far))


def gather_plane(net, buf, t, unit):
    rows, lanes = buf.shape[-2:]
    lane = {None: pl.ds(0, lanes), 0: pl.ds(0, lanes // 2), 1: pl.ds(lanes // 2, lanes // 2)}
    low, high = pl.ds(0, rows // 2), pl.ds(rows // 2, rows // 2)
    c = net.c
    waits = []

    def share_of(ref_of):
        def share(pos):
            slot = net.slot()
            mine, theirs = ref_of(pos, c), ref_of(pos, 1 - c)
            net.start(mine, mine, net.dev(c=1 - c), slot)
            waits.append((theirs, slot))
        return share

    def nothing(pos):
        pass

    def first():
        yield from ring(net, "y", lambda p, h: buf.at[:, p, net.z, c, low, lane[h]], nothing, t, 2.0 + unit)
        yield from ring(
            net, "z", lambda p, h: buf.at[:, :, p, c, low, lane[h]],
            share_of(lambda p, cc: buf.at[:, :, p, cc, low, lane[None]]), t + 5.0 + 2 * unit, 2.0 + 4 * unit,
        )

    def second():
        yield from ring(net, "z", lambda p, h: buf.at[:, net.y, p, c, high, lane[h]], nothing, t, 2.0 + unit)
        yield from ring(
            net, "y", lambda p, h: buf.at[:, p, :, c, high, lane[h]],
            share_of(lambda p, cc: buf.at[:, p, :, cc, high, lane[None]]), t + 9.0 + 4 * unit, 2.0 + 8 * unit,
        )

    yield from merge([first(), second()])
    yield t + 12.0 + 30 * unit
    for ref, slot in waits:
        net.arrive(ref, slot)


def gather_small(net, whole, rows, lanes, t, unit):
    c = net.c
    slots = [net.slot() for _ in range(NZ - 1)]
    mine = whole.at[net.y, net.z, c, rows, lanes]
    for d in (4, 3, 5, 2, 6, 1, 7):
        net.start(mine, mine, net.dev(z=net.at("z", d)), slots[d - 1])
    yield t + 4.0 + 10 * unit
    for d in (1, 7, 2, 6, 3, 5, 4):
        net.arrive(whole.at[net.y, net.at("z", -d), c, rows, lanes], slots[d - 1])
    cuts = {None: pl.ds(0, NZ), 0: pl.ds(0, NZ // 2), 1: pl.ds(NZ // 2, NZ // 2)}
    waits = []

    def share(pos):
        slot = net.slot()
        ref = whole.at[pos, :, c, rows, lanes]
        net.start(ref, ref, net.dev(c=1 - c), slot)
        waits.append((whole.at[pos, :, 1 - c, rows, lanes], slot))

    yield from ring(net, "y", lambda p, h: whole.at[p, cuts[h], c, rows, lanes], share, t + 4.0 + 10 * unit, 2.0 + 6 * unit)
    yield t + 10.0 + 24 * unit
    for ref, slot in waits:
        net.arrive(ref, slot)


def gather_small_turned(net, whole, rows, lanes, t, unit):
    c = net.c
    cuts = {None: lanes, 0: pl.ds(lanes.start, lanes.size // 2), 1: pl.ds(lanes.start + lanes.size // 2, lanes.size // 2)}
    yield from ring(net, "y", lambda p, h: whole.at[p, net.z, c, rows, cuts[h]], lambda at: None, t, 2.2)
    slots = [net.slot() for _ in range(NZ - 1)]
    mine = whole.at[:, net.z, c, rows, lanes]
    for d in (4, 3, 5, 2, 6, 1, 7):
        net.start(mine, mine, net.dev(z=net.at("z", d)), slots[d - 1])
    waits = []

    def share(pos):
        slot = net.slot()
        ref = whole.at[:, pos, c, rows, lanes]
        net.start(ref, ref, net.dev(c=1 - c), slot)
        waits.append((whole.at[:, pos, 1 - c, rows, lanes], slot))

    share(net.z)
    for d in (1, 7, 2, 6, 3, 5, 4):
        yield t + 7.0 + min(d, NZ - d) + 10 * unit
        net.arrive(whole.at[:, net.at("z", -d), c, rows, lanes], slots[d - 1])
        share(net.at("z", -d))
    yield t + 13.0 + 10 * unit
    for ref, slot in waits:
        net.arrive(ref, slot)


def merge(threads):
    live = []
    for thread in threads:
        when = next(thread, None)
        if when is not None:
            live.append([when, len(live), thread])
    while live:
        live.sort(key=lambda item: (item[0], item[1]))
        yield live[0][0]
        when = next(live[0][2], None)
        if when is None:
            live.pop(0)
        else:
            live[0][0] = when


def reduce_plane(net, chain, pay, pair, acc, got1, got2, gotz, t, done):
    c, y, z = net.c, net.y, net.z
    count = got2.shape[-2]
    rw = pl.ds(chain * count, count)
    slot = net.slot()
    net.start(pay.at[1 - c, :, :, rw, :], pair.at[:, :, rw, :], net.dev(c=1 - c), slot)
    yield t + 2.0
    net.arrive(pair.at[:, :, rw, :], slot)

    def add_pair(i, carry):
        acc[i, :, rw, :] = (pay[c, i, :, rw, :].astype(F32) + pair[i, :, rw, :].astype(F32)).astype(BF)
        return carry

    lax.fori_loop(0, NY, add_pair, 0)
    near, over = y + 1 - 2 * lax.rem(y, 2), NY - 1 - y
    half = NZ // 2
    colors = []
    for color, (f, s) in enumerate(((near, over), (over, near))):
        s_of_f = lax.rem(y + 2, NY)
        zs = pl.ds(color * half, half)
        slots = [net.slot() for _ in range(3)]
        net.start(acc.at[s_of_f, zs, rw, :], got1.at[chain, color, 1], net.dev(y=f), slots[1])
        net.start(acc.at[f, zs, rw, :], got1.at[chain, color, 0], net.dev(y=f), slots[0])
        colors.append((f, s, zs, slots))
    yield t + 5.5
    for color, (f, s, zs, slots) in enumerate(colors):
        net.arrive(got1.at[chain, color, 1], slots[1])
        acc[s, zs, rw, :] = (acc[s, zs, rw, :].astype(F32) + got1[chain, color, 1].astype(F32)).astype(BF)
        net.start(acc.at[s, zs, rw, :], got2.at[chain, color], net.dev(y=s), slots[2])
    yield t + 9.5
    for color, (f, s, zs, slots) in enumerate(colors):
        net.arrive(got1.at[chain, color, 0], slots[0])
        net.arrive(got2.at[chain, color], slots[2])
        total = acc[y, zs, rw, :].astype(F32) + got1[chain, color, 0].astype(F32) + got2[chain, color].astype(F32)
        acc[y, zs, rw, :] = total.astype(BF)
    zslots = [net.slot() for _ in range(NZ - 1)]
    for d in (4, 3, 5, 2, 6, 1, 7):
        net.start(acc.at[y, net.at("z", d), rw, :], gotz.at[chain, d - 1], net.dev(z=net.at("z", d)), zslots[d - 1])
    yield t + 16.0
    total = acc[y, z, rw, :].astype(F32)
    for d in range(1, NZ):
        net.arrive(gotz.at[chain, d - 1], zslots[d - 1])
        total = total + gotz[chain, d - 1].astype(F32)
    yield from done(total, t + 16.0)


def small_ends(net, total, tails, scal, xs, t):
    tails[0:8] = total[0:8]
    xs[0] = total[8:16]
    slots = [net.slot() for _ in range(4)]
    net.start(xs.at[0], xs.at[4], net.dev(c=1 - net.c), slots[0])
    for d in (1, 2, 3):
        net.start(xs.at[0], xs.at[d], net.dev(x=net.at("x", d)), slots[d])
    yield t + 18.0
    for d, slot in zip((4, 1, 2, 3), slots):
        net.arrive(xs.at[d], slot)
    tails[8:16] = xs[0] + xs[1] + xs[2] + xs[3]
    scal[...] = jnp.where(jnp.full(scal.shape, net.c) == 1, xs[0], xs[4])


def gather_rows(net, pall):
    rows = pall.shape[1] // 2
    halves = (pl.ds(0, rows), pl.ds(rows, rows))
    x = net.x
    slots = {(d, i): net.slot() for d in (0, 1) for i in range(3)}
    for i in (0, 1):
        for d, way in ((0, 1), (1, -1)):
            ref = pall.at[x, halves[i if d == 0 else 1 - i]]
            net.start(ref, ref, net.dev(x=net.at("x", way)), slots[d, i])
    yield 16.0
    for d, way in ((0, 1), (1, -1)):
        ref = pall.at[net.at("x", -way), halves[d]]
        net.arrive(ref, slots[d, 0])
        net.start(ref, ref, net.dev(x=net.at("x", way)), slots[d, 2])
    yield 40.0
    for d, way in ((0, 1), (1, -1)):
        net.arrive(pall.at[net.at("x", -way), halves[1 - d]], slots[d, 1])
        net.arrive(pall.at[net.at("x", -2), halves[d]], slots[d, 2])


def spread_rows(net, src, place):
    slots = [net.slot() for _ in range(3)]
    for d in (2, 1, 3):
        net.start(src, place(net.x), net.dev(x=net.at("x", d)), slots[d - 1])

    def arrived():
        for d in (1, 3, 2):
            net.arrive(place(net.at("x", -d)), slots[d - 1])

    return arrived


def lanes_of(ref, x, lanes):
    at = pl.ds(pl.multiple_of(x * lanes, lanes), lanes)
    return ref.at[(slice(None),) * (len(ref.shape) - 1) + (at,)]


def front_kernel(
    lead, coef, aux, blk, ham, flat, gamma,
    first, hrho, ham2x, pall, panel, ham2, whole, tails, scal, grow, he_row, hg_row, he_col,
    picks, xs, own2, pay, held, pair, acc, got1, got2, gotz, send, recv,
):
    net = Net(send, recv)
    c, y, z, x = net.c, net.y, net.z, net.x
    peers = [net.dev(x=net.at("x", d)) for d in (1, 2, 3)]
    peers += [net.dev(y=net.at("y", d)) for d in (1, 3)]
    peers += [net.dev(z=net.at("z", d)) for d in range(1, NZ)]
    peers += [net.dev(c=1 - c)]
    net.greet(peers)
    cols, rows = blk.shape[1:]
    arrived = spread_rows(net, blk, lambda at: lanes_of(first, at, rows))
    panel[:, y, z, c] = blk[1:]
    lanes_of(first, x, rows)[...] = blk[...]

    def pick(i, carry):
        at = pl.ds(pl.multiple_of(256 * i, 256), 256)
        here = 256 * i + lax.broadcasted_iota(jnp.int32, (256, flat.shape[1]), 0)
        e = jnp.where(here == flat[...], 1.0, 0.0).astype(BF)
        picks[at, :] = e
        grow[at, :] = by_lead(e, gamma).astype(BF)
        return carry

    def work():
        lax.fori_loop(0, picks.shape[0] // 256, pick, 0)
        g_row = grow[pl.ds(pl.multiple_of(x * rows, rows), rows), :]
        sums(lead, coef, aux, g_row, pall, x, pay, held)
        rows_thread = gather_rows(net, pall)
        start = next(rows_thread)
        chain = reduce_plane(net, 0, pay, pair, acc, got1, got2, gotz, 6.0, gather_sums)
        yield from merge([chain, more(), resumed(rows_thread, start)])

    def gather_sums(total, t):
        whole[y, z, c] = total.astype(BF)
        lanes = total.shape[1]
        yield from gather_small(net, whole, pl.ds(0, 16), pl.ds(0, lanes), t, 0.35)

    def send_ends(total, t):
        yield from small_ends(net, total, tails, scal, xs, t)

    def more():
        yield 7.0
        arrived()
        applied = dot(first[...].reshape(3 * cols, -1), ham[...], 1, 1)
        own2[...] = applied[:cols].astype(BF)
        ham2[0, y, z, c] = own2[...]
        turns = gather_plane(net, ham2, 9.0, 0.4)
        turn = next(turns)
        hrho[...] = applied[cols:]
        hg = dot(first[0], grow[...]).astype(BF)
        lhs = jnp.concatenate([applied[cols:].astype(BF), blk[1:].reshape(2 * cols, rows)], axis=0)
        me = (y * NZ + z) * 2 + c
        g2 = 2 * grow[pl.ds(pl.multiple_of(me * cols, cols), cols), :]
        for i, (sign, p) in enumerate(((1, 1), (-1, 0))):
            left = jnp.concatenate([lhs[p * cols : (p + 1) * cols], lhs[(2 + p) * cols : (3 + p) * cols]], axis=0)
            f = dot(left, sign * jnp.concatenate([g2, -hg], axis=0), 0, 0)
            q = f.shape[1]
            f = f.astype(BF).reshape(NY, NZ, 2, 8, q)
            for cc in range(2):
                pay[cc, :, :, 16:24, i * q : (i + 1) * q] = f[:, :, cc]
        chain = reduce_plane(net, 1, pay, pair, acc, got1, got2, gotz, 11.0, send_ends)
        spread = spread_ham2()
        yield from merge([chain, resumed(turns, turn), spread, spare()])

    def spare():
        yield 13.8
        he_row[...] = dot(ham[...], picks[...]).astype(BF)
        hg_row[...] = dot(ham[...], grow[...])
        he_col[...] = dot(first[0], picks[...]).astype(BF)

    def spread_ham2():
        here = spread_rows(net, own2, lambda at: lanes_of(ham2x, at, rows))
        lanes_of(ham2x, x, rows)[...] = own2[...]
        yield 41.0
        here()

    for _ in merge([gather_plane(net, panel, 1.0, 0.75), work()]):
        pass
    net.finish()


def resumed(thread, start):
    yield start
    yield from thread


def front(lead, coef, aux, blk, ham, flat, gamma):
    cols, lanes = blk.shape[1:]
    n = ham.shape[1]
    vm = pl.BlockSpec(memory_space=pltpu.VMEM)
    sm = pl.BlockSpec(memory_space=pltpu.SMEM)
    sems = 192
    return pl.pallas_call(
        front_kernel,
        out_shape=[
            jax.ShapeDtypeStruct((3, cols, n), BF),
            jax.ShapeDtypeStruct((2 * cols, lanes), F32),
            jax.ShapeDtypeStruct((cols, n), BF),
            jax.ShapeDtypeStruct((4, lanes, aux.size // lanes), BF),
            jax.ShapeDtypeStruct((2, NY, NZ, 2, cols, lanes), BF),
            jax.ShapeDtypeStruct((1, NY, NZ, 2, cols, lanes), BF),
            jax.ShapeDtypeStruct((NY, NZ, 2, 16, lanes), BF),
            jax.ShapeDtypeStruct((16, lanes), F32),
            jax.ShapeDtypeStruct((8, lanes), F32),
            jax.ShapeDtypeStruct((n, flat.shape[1]), BF),
            jax.ShapeDtypeStruct((lanes, flat.shape[1]), BF),
            jax.ShapeDtypeStruct((lanes, flat.shape[1]), F32),
            jax.ShapeDtypeStruct((cols, flat.shape[1]), BF),
        ],
        in_specs=[sm, sm] + [vm] * 5,
        out_specs=[vm] * 13,
        scratch_shapes=[
            pltpu.VMEM((n, flat.shape[1]), BF),
            pltpu.VMEM((5, 8, lanes), F32),
            pltpu.VMEM((cols, lanes), BF),
            pltpu.VMEM((2, NY, NZ, 32, lanes), BF),
            pltpu.VMEM((lanes, lanes), BF),
            pltpu.VMEM((NY, NZ, 32, lanes), BF),
            pltpu.VMEM((NY, NZ, 32, lanes), BF),
            pltpu.VMEM((2, 2, 2, NZ // 2, 16, lanes), BF),
            pltpu.VMEM((2, 2, NZ // 2, 16, lanes), BF),
            pltpu.VMEM((2, NZ - 1, 16, lanes), BF),
            pltpu.SemaphoreType.DMA((sems,)),
            pltpu.SemaphoreType.DMA((sems,)),
        ],
        compiler_params=pltpu.CompilerParams(collective_id=1, has_side_effects=True, vmem_limit_bytes=30 * 1024 * 1024),
        cost_estimate=pl.CostEstimate(flops=10**11, bytes_accessed=2**24, transcendentals=0),
        name="front",
    )(lead, coef, aux, blk, ham, flat, gamma)


def back_kernel(blk, tails, out, n_all, send, recv):
    net = Net(send, recv)
    peers = [net.dev(x=net.at("x", d)) for d in (1, 2, 3)]
    peers += [net.dev(y=net.at("y", d)) for d in (1, 3)]
    peers += [net.dev(z=net.at("z", d)) for d in range(1, NZ)]
    peers += [net.dev(c=1 - net.c)]
    net.greet(peers)
    lanes = blk.shape[1]
    lanes_of(out, net.x, lanes)[...] = blk[...]
    n_all[net.y, net.z, net.c] = tails[...].astype(BF)
    half = lanes // 2
    cuts = {None: (0, lanes), 0: (0, half), 1: (half, half)}

    def part(at, h):
        first, width = cuts[h]
        return out.at[:, pl.ds(pl.multiple_of(at * lanes + first, half), width)]

    for _ in merge([
        gather_small(net, n_all, pl.ds(0, 16), pl.ds(0, half), 0.0, 0.2),
        gather_small_turned(net, n_all, pl.ds(0, 16), pl.ds(half, half), 0.0, 0.3),
        ring(net, "x", part, lambda at: None, 0.0, 4.0),
    ]):
        pass
    net.finish()


def back(blk, tails):
    lanes = blk.shape[1]
    vm = pl.BlockSpec(memory_space=pltpu.VMEM)
    return pl.pallas_call(
        back_kernel,
        out_shape=[
            jax.ShapeDtypeStruct((blk.shape[0], 4 * lanes), BF),
            jax.ShapeDtypeStruct((NY, NZ, 2, 16, lanes), BF),
        ],
        in_specs=[vm] * 2,
        out_specs=[vm] * 2,
        scratch_shapes=[
            pltpu.SemaphoreType.DMA((48,)),
            pltpu.SemaphoreType.DMA((48,)),
        ],
        compiler_params=pltpu.CompilerParams(collective_id=2, has_side_effects=True, vmem_limit_bytes=8 * 1024 * 1024),
        cost_estimate=pl.CostEstimate(flops=3 * 10**10, bytes_accessed=2**20, transcendentals=0),
        name="back",
    )(blk, tails)


def sums(lead, coef, aux, g_row, pall, x, pay, held):
    q = g_row.shape[1]
    coupled = aux.shape[1]
    modes = aux.shape[0] // (2 * held.shape[0])
    leads = q // coupled
    hot = [[jnp.where(lead[k] == l, 1.0, 0.0) for l in range(leads)] for k in range(modes)]
    level, width, re, im, occ = ([coef[i, k] for k in range(modes)] for i in range(5))

    def chunk(t, carry):
        rows = pl.ds(pl.multiple_of(32 * t, 32), 32)
        part = [aux[pl.ds(pl.multiple_of(32 * t * 2 * modes, 32) + i, 32, stride=2 * modes), :] for i in range(2 * modes)]
        pall[x, rows, :] = jnp.concatenate(part, axis=1).astype(BF)
        turned = []
        for k in range(modes):
            turned.append(-width[k] * part[2 * k] - level[k] * part[2 * k + 1])
            turned.append(level[k] * part[2 * k] - width[k] * part[2 * k + 1])

        def summed(values):
            out = []
            for p in range(2):
                for l in range(leads):
                    total = hot[0][l] * values[p]
                    for k in range(1, modes):
                        total = total + hot[k][l] * values[2 * k + p]
                    out.append(total)
            return jnp.concatenate(out, axis=1)

        l_sum = summed(part)
        held[rows, :] = l_sum.astype(BF)
        for i, a in enumerate((l_sum, summed(turned))):
            a = a.reshape(2, 2, 8, 2 * q).astype(BF)
            for c in range(2):
                pay[c, t // 4, pl.ds(2 * lax.rem(t, 4), 2), pl.ds(8 * i, 8), :] = a[:, c]
        return carry

    lax.fori_loop(0, held.shape[0] // 32, chunk, 0)
    n_re = dot(held[:, :q], g_row, 0, 0)
    n_im = -dot(held[:, q:], g_row, 0, 0)
    n = jnp.concatenate([n_re, n_im], axis=1).astype(BF)
    pay[0, :, :, 24:32, :] = n.reshape(NY, NZ, 8, 2 * q)
    lane = lax.broadcasted_iota(jnp.int32, (8, 2 * q), 1)
    scal = jnp.zeros((8, 2 * q), F32)
    for i, weights in enumerate((re, im, [re[k] * occ[k] for k in range(modes)], [im[k] * occ[k] for k in range(modes)])):
        for l in range(leads):
            scal = jnp.where(lane == i * leads + l, sum(weights[k] * hot[k][l] for k in range(modes)), scal)
    pay[1, :, :, 24:32, :] = jnp.broadcast_to(scal.astype(BF), (NY, NZ, 8, 2 * q))


def modes_kernel(lead, coef, aux, ham, ham2, pi, src, u, g, hg, out, hp, h2p, turned):
    k = pl.program_id(0)

    @pl.when(k == 0)
    def _():
        for i in range(0, ham2.shape[0], 512):
            turned[:, i : i + 512] = ham2[i : i + 512, :].T

    coupled = aux.shape[1]
    rows = ham.shape[0]
    modes = aux.shape[0] // (2 * rows)
    q = g.shape[1]
    hp[...] = dot(ham[...], pi[...])
    h2p[...] = dot(turned[...], pi[...])
    level, width, wr, wi, occ = (coef[i, k] for i in range(5))
    first = pl.multiple_of(lead[k] * coupled, coupled)
    re, im = pl.ds(first, coupled), pl.ds(pl.multiple_of(q + first, coupled), coupled)
    lr, li = -width, level
    ar, ai = 3 + 2 * H2 * lr, 2 * H2 * li
    cr = 3 * lr + 2 * H2 * (lr * lr - li * li)
    ci = 3 * li + 4 * H2 * lr * li
    er, ei = 4 * H2 * li, -3 - 4 * H2 * lr
    size = 64

    def chunk(t, carry):
        at = pl.ds(pl.multiple_of(size * t, size), size)
        gk, hgk = occ * g[at, re].astype(F32), 2 * H2 * occ * hg[at, re]
        br, bi = src[at, re] - gk, src[at, im] - gk
        tr = ar * br - ai * bi + u[at, re] - hgk
        ti = ar * bi + ai * br + u[at, im] + hgk
        start = pl.multiple_of(size * t * 2 * modes, size) + 2 * k
        at_re = pl.ds(start, size, stride=2 * modes)
        at_im = pl.ds(start + 1, size, stride=2 * modes)
        pr, pim = aux[at_re, :], aux[at_im, :]
        hr, hi = hp[at, :coupled], hp[at, coupled:]
        out[at_re, :] = cr * pr - ci * pim + er * hr - ei * hi - 2 * H2 * h2p[at, :coupled] + wr * tr - wi * ti
        out[at_im, :] = cr * pim + ci * pr + er * hi + ei * hr - 2 * H2 * h2p[at, coupled:] + wr * ti + wi * tr
        return carry

    lax.fori_loop(0, rows // size, chunk, 0)


def advance_modes(lead, coef, aux, ham, ham2, pi, src, u, g, hg):
    rows, n = ham.shape
    coupled = aux.shape[1]
    modes = aux.shape[0] // (2 * rows)
    sm = pl.BlockSpec(memory_space=pltpu.SMEM)

    def whole(a):
        return pl.BlockSpec(a.shape, lambda k: (0,) * a.ndim)

    return pl.pallas_call(
        modes_kernel,
        grid=(modes,),
        out_shape=jax.ShapeDtypeStruct(aux.shape, F32),
        in_specs=[sm, sm, whole(aux), whole(ham), whole(ham2), pl.BlockSpec((n, 2 * coupled), lambda k: (0, k))]
        + [whole(a) for a in (src, u, g, hg)],
        out_specs=whole(aux),
        scratch_shapes=[pltpu.VMEM((rows, 2 * coupled), F32)] * 2 + [pltpu.VMEM((rows, n), BF)],
        compiler_params=pltpu.CompilerParams(vmem_limit_bytes=28 * 1024 * 1024),
        cost_estimate=pl.CostEstimate(flops=4 * rows * n * 2 * coupled * modes, bytes_accessed=16 * 1024 * 1024, transcendentals=0),
        name="modes",
    )(lead, coef, aux, ham, ham2, pi, src, u, g, hg)


def by_lead(x, gamma):
    leads, coupled = gamma.shape[:2]
    return jnp.concatenate(
        [dot(x[:, l * coupled : (l + 1) * coupled], gamma[l]) for l in range(leads)], axis=1
    )


def shards(density, auxiliary, hamiltonian, coupling, lead_index, mode_level, mode_width, residue, occupation, lead_gamma):
    rows, cols = density.shape[1:]
    n = hamiltonian.shape[1]
    leads, coupled = coupling.shape
    q = leads * coupled
    modes = auxiliary.shape[1]
    n_mode = lax.axis_size("mode")
    n_row = lax.axis_size("row")
    x_pos, m_pos = lax.axis_index("row"), lax.axis_index("mode")
    row_start, col_start = x_pos * rows, m_pos * cols
    flat = coupling.reshape(-1)

    e_row = (row_start + jnp.arange(rows, dtype=jnp.int32)[:, None] == flat[None, :]).astype(BF)
    e_col = (col_start + jnp.arange(cols, dtype=jnp.int32)[:, None] == flat[None, :]).astype(BF)
    rho_t = jnp.swapaxes(density, 1, 2).astype(BF).reshape(2 * cols, rows)
    ham_ct = jnp.swapaxes(lax.dynamic_slice_in_dim(hamiltonian, col_start, cols, 1), 0, 1)

    coef = jnp.stack([mode_level, mode_width, residue[:, 0], residue[:, 1], occupation])
    aux = auxiliary.reshape(-1, coupled)
    blk = jnp.concatenate([ham_ct, rho_t], axis=0).reshape(3, cols, rows)
    first, hrho_t, ham2_c, pi_all, panel, ham2_all, whole, tails, scal, grow_full, he_row_b, hg_row, he_col = front(
        lead_index, coef, aux, blk, hamiltonian, flat[None], lead_gamma
    )
    g_row = lax.dynamic_slice_in_dim(grow_full, row_start, rows, 0)
    ham_c = first[0]
    piece = rows // n_mode
    pi_all = pi_all.reshape(n, -1)
    panel = panel.reshape(2, n, rows)
    ham2_all = ham2_all.reshape(n, rows)
    whole = whole.reshape(n_mode, 2 * piece, 2 * q)
    l1_b = whole[:, :piece].reshape(rows, 2 * q)
    m1 = whole[:, piece : 2 * piece].reshape(rows, 2 * q).astype(F32)
    scal = scal[0]
    w_sum, v_sum = scal[: 2 * leads], scal[2 * leads : 4 * leads]

    src = dot(panel, grow_full, 1, 0)
    src = jnp.concatenate([src[0], src[1]], axis=1)
    w_q = jnp.repeat(w_sum, coupled)
    v_q = jnp.repeat(v_sum, coupled)
    s_re, s_im = src[:, :q], src[:, q:]
    g_row_f = g_row.astype(F32)
    drive = jnp.concatenate(
        [w_q[:q] * s_re - w_q[q:] * s_im - (v_q[:q] - v_q[q:]) * g_row_f, w_q[:q] * s_im + w_q[q:] * s_re - (v_q[:q] + v_q[q:]) * g_row_f], axis=1
    )
    x_row = (3.0 * l1_b.astype(F32) + 2 * H2 * (m1 + drive)).astype(BF)
    p1 = jnp.concatenate([dot(e_col, l1_b[:, p * q : (p + 1) * q], 1, 1) for p in range(2)], 0)
    xe = jnp.concatenate([dot(e_col, x_row[:, p * q : (p + 1) * q], 1, 1) for p in range(2)], 0)
    rhoh_t = jnp.swapaxes(dot(jnp.concatenate([ham_c, ham2_c], 0), panel, 1, 1), 0, 1)
    rhoh_t, rhoh2_t = (rhoh_t[:, i * cols : (i + 1) * cols].reshape(2 * cols, rows) for i in range(2))
    y = hrho_t - 2.0 * rhoh_t + 2.0 * jnp.concatenate([-p1[cols:], p1[:cols]], 0)
    z = dot(lax.dynamic_slice_in_dim(ham_c, row_start, rows, 1), l1_b)
    owner = col_start // rows
    own_l = lax.dynamic_slice_in_dim(l1_b, col_start - owner * rows, cols, 0)
    own_x = lax.dynamic_slice_in_dim(x_row, col_start - owner * rows, cols, 0)
    mask = (x_pos == owner).astype(BF)
    second, n_all = back(jnp.concatenate([y.astype(BF), z.astype(BF), own_l * mask, own_x * mask], 0), tails)
    f_all = n_all[..., :8, :].reshape(rows, 2 * q).astype(F32)
    n_all = n_all[:, :, 0, 8:].reshape(q, 2 * q)
    third = second[2 * cols :].astype(F32)
    third = sum(third[:, i * rows : (i + 1) * rows] for i in range(n_row))
    z, l_c, x_c = third[:cols], third[cols : 2 * cols], third[2 * cols :]
    hy = dot(second[: 2 * cols], hamiltonian, 1, 1)
    b_re = x_c[:, :q] + 4 * H2 * z[:, q:]
    b_im = -x_c[:, q:] + 4 * H2 * z[:, :q]
    back_re = dot(b_re.astype(BF), e_row, 1, 1)
    back_im = dot(b_im.astype(BF), e_row, 1, 1)
    l_cb = l_c.astype(BF)
    c1_re, c1_im = dot(l_cb[:, :q], he_row_b, 1, 1), -dot(l_cb[:, q:], he_row_b, 1, 1)
    c2_re, c2_im = dot(he_col, l1_b[:, :q], 1, 1), dot(he_col, l1_b[:, q:], 1, 1)
    d_re, d_im = c1_re - c2_re, c1_im - c2_im
    comm = hrho_t - rhoh_t
    base = -2 * H2 * (hy + rhoh2_t) + xe
    out_re = 3.0 * comm[cols:] + base[:cols] + back_re + 2 * H2 * d_im
    out_im = -3.0 * comm[:cols] + base[cols:] + back_im - 2 * H2 * d_re
    density_rate = jnp.swapaxes(jnp.stack([out_re, out_im]), 1, 2)

    lg = jnp.concatenate([by_lead(l1_b[:, p * q : (p + 1) * q], lead_gamma) for p in range(2)], 1)
    u = 2 * H2 * (f_all + lg + dot(e_row, n_all))
    auxiliary_rate = advance_modes(
        lead_index, coef, aux, hamiltonian, ham2_all, pi_all, src, u, g_row, hg_row
    ).reshape(auxiliary.shape)
    return density_rate, auxiliary_rate


def solution(mesh):
    in_specs = (
        P(None, "row", "mode"),
        P("row", "mode", None, None),
        P("row", None),
        P(),
        P("mode"),
        P("mode"),
        P("mode"),
        P("mode", None),
        P("mode"),
        P(),
    )
    out_specs = (P(None, "row", "mode"), P("row", "mode", None, None))
    return jax.shard_map(shards, mesh=mesh, in_specs=in_specs, out_specs=out_specs, check_vma=False)
```

```python
import jax
import jax.numpy as jnp
from jax import lax
from jax.experimental import pallas as pl
from jax.experimental.pallas import tpu as pltpu
from jax.sharding import PartitionSpec as P

H2 = 0.05
F32 = jnp.float32
BF = jnp.bfloat16


def dot(a, b, ca=1, cb=0):
    return lax.dot_general(a, b, (((ca,), (cb,)), ((), ())), preferred_element_type=F32)


MESH = pl.DeviceIdType.MESH
NY, NZ = 4, 8


class Net:
    def __init__(self, send, recv):
        self.send, self.recv, self.used, self.sent = send, recv, 0, []
        m = lax.axis_index("mode")
        self.x = lax.axis_index("row")
        self.c, self.z, self.y = lax.rem(m, 2), lax.rem(m // 2, NZ), m // (2 * NZ)

    def dev(self, y=None, z=None, c=None, x=None):
        y = self.y if y is None else y
        z = self.z if z is None else z
        c = self.c if c is None else c
        return {"mode": (y * NZ + z) * 2 + c, "row": self.x if x is None else x}

    def at(self, name, d):
        size = {"x": 4, "y": NY, "z": NZ}[name]
        return lax.rem(getattr(self, name) + (d % size), size)

    def slot(self):
        self.used += 1
        return self.used - 1

    def start(self, src, dst, to, slot):
        copy = pltpu.make_async_remote_copy(
            src_ref=src, dst_ref=dst, send_sem=self.send.at[slot], recv_sem=self.recv.at[slot], device_id=to, device_id_type=MESH
        )
        copy.start()
        self.sent.append(copy)

    def arrive(self, ref, slot):
        pltpu.make_async_remote_copy(
            src_ref=ref, dst_ref=ref, send_sem=self.send.at[slot], recv_sem=self.recv.at[slot],
            device_id=self.dev(c=1 - self.c), device_id_type=MESH,
        ).wait_recv()

    def finish(self):
        for copy in self.sent:
            copy.wait_send()

    def greet(self, peers):
        barrier = pltpu.get_barrier_semaphore()
        for peer in peers:
            pl.semaphore_signal(barrier, inc=1, device_id=peer, device_id_type=MESH)
        pl.semaphore_wait(barrier, len(peers))


def ring(net, name, part, share, t, step):
    size = {"x": 4, "y": NY, "z": NZ}[name]
    far = size // 2
    slots = {(d, s): net.slot() for s in range(1, far + 1) for d in (1, -1)}
    at = lambda d: net.at(name, d)
    for d in (1, -1):
        net.start(part(at(0), None), part(at(0), None), net.dev(**{name: at(d)}), slots[d, 1])
    share(at(0))
    for s in range(1, far + 1):
        yield t + s * step
        for d in (1, -1):
            half = None if s < far else (d + 1) // 2
            net.arrive(part(at(-d * s), half), slots[d, s])
            if s < far:
                half = None if s + 1 < far else (d + 1) // 2
                net.start(part(at(-d * s), half), part(at(-d * s), half), net.dev(**{name: at(d)}), slots[d, s + 1])
        if s < far:
            share(at(s))
            share(at(-s))
        else:
            share(at(far))


def gather_plane(net, buf, t, unit):
    rows, lanes = buf.shape[-2:]
    lane = {None: pl.ds(0, lanes), 0: pl.ds(0, lanes // 2), 1: pl.ds(lanes // 2, lanes // 2)}
    low, high = pl.ds(0, rows // 2), pl.ds(rows // 2, rows // 2)
    c = net.c
    waits = []

    def share_of(ref_of):
        def share(pos):
            slot = net.slot()
            mine, theirs = ref_of(pos, c), ref_of(pos, 1 - c)
            net.start(mine, mine, net.dev(c=1 - c), slot)
            waits.append((theirs, slot))
        return share

    def nothing(pos):
        pass

    def first():
        yield from ring(net, "y", lambda p, h: buf.at[:, p, net.z, c, low, lane[h]], nothing, t, 2.0 + unit)
        yield from ring(
            net, "z", lambda p, h: buf.at[:, :, p, c, low, lane[h]],
            share_of(lambda p, cc: buf.at[:, :, p, cc, low, lane[None]]), t + 5.0 + 2 * unit, 2.0 + 4 * unit,
        )

    def second():
        yield from ring(net, "z", lambda p, h: buf.at[:, net.y, p, c, high, lane[h]], nothing, t, 2.0 + unit)
        yield from ring(
            net, "y", lambda p, h: buf.at[:, p, :, c, high, lane[h]],
            share_of(lambda p, cc: buf.at[:, p, :, cc, high, lane[None]]), t + 9.0 + 4 * unit, 2.0 + 8 * unit,
        )

    yield from merge([first(), second()])
    yield t + 12.0 + 30 * unit
    for ref, slot in waits:
        net.arrive(ref, slot)


def gather_small(net, whole, rows, lanes, t, unit):
    c = net.c
    slots = [net.slot() for _ in range(NZ - 1)]
    mine = whole.at[net.y, net.z, c, rows, lanes]
    for d in (4, 3, 5, 2, 6, 1, 7):
        net.start(mine, mine, net.dev(z=net.at("z", d)), slots[d - 1])
    yield t + 4.0 + 10 * unit
    for d in (1, 7, 2, 6, 3, 5, 4):
        net.arrive(whole.at[net.y, net.at("z", -d), c, rows, lanes], slots[d - 1])
    cuts = {None: pl.ds(0, NZ), 0: pl.ds(0, NZ // 2), 1: pl.ds(NZ // 2, NZ // 2)}
    waits = []

    def share(pos):
        slot = net.slot()
        ref = whole.at[pos, :, c, rows, lanes]
        net.start(ref, ref, net.dev(c=1 - c), slot)
        waits.append((whole.at[pos, :, 1 - c, rows, lanes], slot))

    yield from ring(net, "y", lambda p, h: whole.at[p, cuts[h], c, rows, lanes], share, t + 4.0 + 10 * unit, 2.0 + 6 * unit)
    yield t + 10.0 + 24 * unit
    for ref, slot in waits:
        net.arrive(ref, slot)


def gather_small_turned(net, whole, rows, lanes, t, unit):
    c = net.c
    cuts = {None: lanes, 0: pl.ds(lanes.start, lanes.size // 2), 1: pl.ds(lanes.start + lanes.size // 2, lanes.size // 2)}
    yield from ring(net, "y", lambda p, h: whole.at[p, net.z, c, rows, cuts[h]], lambda at: None, t, 2.2)
    slots = [net.slot() for _ in range(NZ - 1)]
    mine = whole.at[:, net.z, c, rows, lanes]
    for d in (4, 3, 5, 2, 6, 1, 7):
        net.start(mine, mine, net.dev(z=net.at("z", d)), slots[d - 1])
    waits = []

    def share(pos):
        slot = net.slot()
        ref = whole.at[:, pos, c, rows, lanes]
        net.start(ref, ref, net.dev(c=1 - c), slot)
        waits.append((whole.at[:, pos, 1 - c, rows, lanes], slot))

    share(net.z)
    for d in (1, 7, 2, 6, 3, 5, 4):
        yield t + 7.0 + min(d, NZ - d) + 10 * unit
        net.arrive(whole.at[:, net.at("z", -d), c, rows, lanes], slots[d - 1])
        share(net.at("z", -d))
    yield t + 13.0 + 10 * unit
    for ref, slot in waits:
        net.arrive(ref, slot)


def merge(threads):
    live = []
    for thread in threads:
        when = next(thread, None)
        if when is not None:
            live.append([when, len(live), thread])
    while live:
        live.sort(key=lambda item: (item[0], item[1]))
        yield live[0][0]
        when = next(live[0][2], None)
        if when is None:
            live.pop(0)
        else:
            live[0][0] = when


def reduce_plane(net, chain, pay, pair, acc, got1, got2, gotz, t, done):
    c, y, z = net.c, net.y, net.z
    count = got2.shape[-2]
    rw = pl.ds(chain * count, count)
    slot = net.slot()
    net.start(pay.at[1 - c, :, :, rw, :], pair.at[:, :, rw, :], net.dev(c=1 - c), slot)
    yield t + 2.0
    net.arrive(pair.at[:, :, rw, :], slot)

    def add_pair(i, carry):
        acc[i, :, rw, :] = (pay[c, i, :, rw, :].astype(F32) + pair[i, :, rw, :].astype(F32)).astype(BF)
        return carry

    lax.fori_loop(0, NY, add_pair, 0)
    near, over = y + 1 - 2 * lax.rem(y, 2), NY - 1 - y
    half = NZ // 2
    colors = []
    for color, (f, s) in enumerate(((near, over), (over, near))):
        s_of_f = lax.rem(y + 2, NY)
        zs = pl.ds(color * half, half)
        slots = [net.slot() for _ in range(3)]
        net.start(acc.at[s_of_f, zs, rw, :], got1.at[chain, color, 1], net.dev(y=f), slots[1])
        net.start(acc.at[f, zs, rw, :], got1.at[chain, color, 0], net.dev(y=f), slots[0])
        colors.append((f, s, zs, slots))
    yield t + 5.5
    for color, (f, s, zs, slots) in enumerate(colors):
        net.arrive(got1.at[chain, color, 1], slots[1])
        acc[s, zs, rw, :] = (acc[s, zs, rw, :].astype(F32) + got1[chain, color, 1].astype(F32)).astype(BF)
        net.start(acc.at[s, zs, rw, :], got2.at[chain, color], net.dev(y=s), slots[2])
    yield t + 9.5
    for color, (f, s, zs, slots) in enumerate(colors):
        net.arrive(got1.at[chain, color, 0], slots[0])
        net.arrive(got2.at[chain, color], slots[2])
        total = acc[y, zs, rw, :].astype(F32) + got1[chain, color, 0].astype(F32) + got2[chain, color].astype(F32)
        acc[y, zs, rw, :] = total.astype(BF)
    zslots = [net.slot() for _ in range(NZ - 1)]
    for d in (4, 3, 5, 2, 6, 1, 7):
        net.start(acc.at[y, net.at("z", d), rw, :], gotz.at[chain, d - 1], net.dev(z=net.at("z", d)), zslots[d - 1])
    yield t + 16.0
    total = acc[y, z, rw, :].astype(F32)
    for d in range(1, NZ):
        net.arrive(gotz.at[chain, d - 1], zslots[d - 1])
        total = total + gotz[chain, d - 1].astype(F32)
    yield from done(total, t + 16.0)


def small_ends(net, total, tails, scal, xs, t):
    tails[0:8] = total[0:8]
    xs[0] = total[8:16]
    slots = [net.slot() for _ in range(4)]
    net.start(xs.at[0], xs.at[4], net.dev(c=1 - net.c), slots[0])
    for d in (1, 2, 3):
        net.start(xs.at[0], xs.at[d], net.dev(x=net.at("x", d)), slots[d])
    yield t + 18.0
    for d, slot in zip((4, 1, 2, 3), slots):
        net.arrive(xs.at[d], slot)
    tails[8:16] = xs[0] + xs[1] + xs[2] + xs[3]
    scal[...] = jnp.where(jnp.full(scal.shape, net.c) == 1, xs[0], xs[4])


def gather_rows(net, pall):
    rows = pall.shape[1] // 2
    halves = (pl.ds(0, rows), pl.ds(rows, rows))
    x = net.x
    slots = {(d, i): net.slot() for d in (0, 1) for i in range(3)}
    for i in (0, 1):
        for d, way in ((0, 1), (1, -1)):
            ref = pall.at[x, halves[i if d == 0 else 1 - i]]
            net.start(ref, ref, net.dev(x=net.at("x", way)), slots[d, i])
    yield 16.0
    for d, way in ((0, 1), (1, -1)):
        ref = pall.at[net.at("x", -way), halves[d]]
        net.arrive(ref, slots[d, 0])
        net.start(ref, ref, net.dev(x=net.at("x", way)), slots[d, 2])
    yield 40.0
    for d, way in ((0, 1), (1, -1)):
        net.arrive(pall.at[net.at("x", -way), halves[1 - d]], slots[d, 1])
        net.arrive(pall.at[net.at("x", -2), halves[d]], slots[d, 2])


def spread_rows(net, src, place):
    slots = [net.slot() for _ in range(3)]
    for d in (2, 1, 3):
        net.start(src, place(net.x), net.dev(x=net.at("x", d)), slots[d - 1])

    def arrived():
        for d in (1, 3, 2):
            net.arrive(place(net.at("x", -d)), slots[d - 1])

    return arrived


def lanes_of(ref, x, lanes):
    at = pl.ds(pl.multiple_of(x * lanes, lanes), lanes)
    return ref.at[(slice(None),) * (len(ref.shape) - 1) + (at,)]


def front_kernel(
    lead, coef, aux, blk, ham, flat, gamma,
    first, hrho, ham2x, pall, panel, ham2, whole, tails, scal, grow, he_row, hg_row, he_col,
    picks, xs, own2, pay, held, pair, acc, got1, got2, gotz, send, recv,
):
    net = Net(send, recv)
    c, y, z, x = net.c, net.y, net.z, net.x
    peers = [net.dev(x=net.at("x", d)) for d in (1, 2, 3)]
    peers += [net.dev(y=net.at("y", d)) for d in (1, 3)]
    peers += [net.dev(z=net.at("z", d)) for d in range(1, NZ)]
    peers += [net.dev(c=1 - c)]
    net.greet(peers)
    cols, rows = blk.shape[1:]
    arrived = spread_rows(net, blk, lambda at: lanes_of(first, at, rows))
    panel[:, y, z, c] = blk[1:]
    lanes_of(first, x, rows)[...] = blk[...]

    def pick(i, carry):
        at = pl.ds(pl.multiple_of(256 * i, 256), 256)
        here = 256 * i + lax.broadcasted_iota(jnp.int32, (256, flat.shape[1]), 0)
        e = jnp.where(here == flat[...], 1.0, 0.0).astype(BF)
        picks[at, :] = e
        grow[at, :] = by_lead(e, gamma).astype(BF)
        return carry

    def work():
        lax.fori_loop(0, picks.shape[0] // 256, pick, 0)
        g_row = grow[pl.ds(pl.multiple_of(x * rows, rows), rows), :]
        sums(lead, coef, aux, g_row, pall, x, pay, held)
        rows_thread = gather_rows(net, pall)
        start = next(rows_thread)
        chain = reduce_plane(net, 0, pay, pair, acc, got1, got2, gotz, 6.0, gather_sums)
        yield from merge([chain, more(), resumed(rows_thread, start)])

    def gather_sums(total, t):
        whole[y, z, c] = total.astype(BF)
        lanes = total.shape[1]
        yield from gather_small(net, whole, pl.ds(0, 16), pl.ds(0, lanes), t, 0.35)

    def send_ends(total, t):
        yield from small_ends(net, total, tails, scal, xs, t)

    def more():
        yield 7.0
        arrived()
        applied = dot(first[...].reshape(3 * cols, -1), ham[...], 1, 1)
        own2[...] = applied[:cols].astype(BF)
        ham2[0, y, z, c] = own2[...]
        turns = gather_plane(net, ham2, 9.0, 0.4)
        turn = next(turns)
        hrho[...] = applied[cols:]
        hg = dot(first[0], grow[...]).astype(BF)
        lhs = jnp.concatenate([applied[cols:].astype(BF), blk[1:].reshape(2 * cols, rows)], axis=0)
        me = (y * NZ + z) * 2 + c
        g2 = 2 * grow[pl.ds(pl.multiple_of(me * cols, cols), cols), :]
        for i, (sign, p) in enumerate(((1, 1), (-1, 0))):
            left = jnp.concatenate([lhs[p * cols : (p + 1) * cols], lhs[(2 + p) * cols : (3 + p) * cols]], axis=0)
            f = dot(left, sign * jnp.concatenate([g2, -hg], axis=0), 0, 0)
            q = f.shape[1]
            f = f.astype(BF).reshape(NY, NZ, 2, 8, q)
            for cc in range(2):
                pay[cc, :, :, 16:24, i * q : (i + 1) * q] = f[:, :, cc]
        chain = reduce_plane(net, 1, pay, pair, acc, got1, got2, gotz, 11.0, send_ends)
        spread = spread_ham2()
        yield from merge([chain, resumed(turns, turn), spread, spare()])

    def spare():
        yield 13.8
        he_row[...] = dot(ham[...], picks[...]).astype(BF)
        hg_row[...] = dot(ham[...], grow[...])
        he_col[...] = dot(first[0], picks[...]).astype(BF)

    def spread_ham2():
        here = spread_rows(net, own2, lambda at: lanes_of(ham2x, at, rows))
        lanes_of(ham2x, x, rows)[...] = own2[...]
        yield 41.0
        here()

    for _ in merge([gather_plane(net, panel, 1.0, 0.75), work()]):
        pass
    net.finish()


def resumed(thread, start):
    yield start
    yield from thread


def front(lead, coef, aux, blk, ham, flat, gamma):
    cols, lanes = blk.shape[1:]
    n = ham.shape[1]
    vm = pl.BlockSpec(memory_space=pltpu.VMEM)
    sm = pl.BlockSpec(memory_space=pltpu.SMEM)
    sems = 192
    return pl.pallas_call(
        front_kernel,
        out_shape=[
            jax.ShapeDtypeStruct((3, cols, n), BF),
            jax.ShapeDtypeStruct((2 * cols, lanes), F32),
            jax.ShapeDtypeStruct((cols, n), BF),
            jax.ShapeDtypeStruct((4, lanes, aux.size // lanes), BF),
            jax.ShapeDtypeStruct((2, NY, NZ, 2, cols, lanes), BF),
            jax.ShapeDtypeStruct((1, NY, NZ, 2, cols, lanes), BF),
            jax.ShapeDtypeStruct((NY, NZ, 2, 16, lanes), BF),
            jax.ShapeDtypeStruct((16, lanes), F32),
            jax.ShapeDtypeStruct((8, lanes), F32),
            jax.ShapeDtypeStruct((n, flat.shape[1]), BF),
            jax.ShapeDtypeStruct((lanes, flat.shape[1]), BF),
            jax.ShapeDtypeStruct((lanes, flat.shape[1]), F32),
            jax.ShapeDtypeStruct((cols, flat.shape[1]), BF),
        ],
        in_specs=[sm, sm] + [vm] * 5,
        out_specs=[vm] * 13,
        scratch_shapes=[
            pltpu.VMEM((n, flat.shape[1]), BF),
            pltpu.VMEM((5, 8, lanes), F32),
            pltpu.VMEM((cols, lanes), BF),
            pltpu.VMEM((2, NY, NZ, 32, lanes), BF),
            pltpu.VMEM((lanes, lanes), BF),
            pltpu.VMEM((NY, NZ, 32, lanes), BF),
            pltpu.VMEM((NY, NZ, 32, lanes), BF),
            pltpu.VMEM((2, 2, 2, NZ // 2, 16, lanes), BF),
            pltpu.VMEM((2, 2, NZ // 2, 16, lanes), BF),
            pltpu.VMEM((2, NZ - 1, 16, lanes), BF),
            pltpu.SemaphoreType.DMA((sems,)),
            pltpu.SemaphoreType.DMA((sems,)),
        ],
        compiler_params=pltpu.CompilerParams(collective_id=1, has_side_effects=True, vmem_limit_bytes=30 * 1024 * 1024),
        cost_estimate=pl.CostEstimate(flops=10**11, bytes_accessed=2**24, transcendentals=0),
        name="front",
    )(lead, coef, aux, blk, ham, flat, gamma)


def products(ham, ham2, pi, hp, h2p, turned):
    size, deep = 256, 512
    pieces = pi.shape[1] // size

    def turn(i):
        turned[:, i * deep : (i + 1) * deep] = ham2[i * deep : (i + 1) * deep, :].T

    def times(left, out, k):
        out[:, k * size : (k + 1) * size] = dot(left[...], pi[:, k * size : (k + 1) * size])

    steps = [lambda k=k: times(ham, hp, k) for k in range(pieces)]
    steps += [lambda i=i: turn(i) for i in range(ham2.shape[0] // deep)]
    steps += [lambda k=k: times(turned, h2p, k) for k in range(pieces)]
    for step, t in zip(steps, (0.5, 0.6, 0.7, 2.3, 2.4, 4.5, 4.6, 4.7, 6.1, 6.2, 8.1, 9.5)):
        yield t
        step()


def back_kernel(blk, tails, ham, ham2, pi, out, n_all, hp, h2p, turned, send, recv):
    net = Net(send, recv)
    peers = [net.dev(x=net.at("x", d)) for d in (1, 2, 3)]
    peers += [net.dev(y=net.at("y", d)) for d in (1, 3)]
    peers += [net.dev(z=net.at("z", d)) for d in range(1, NZ)]
    peers += [net.dev(c=1 - net.c)]
    net.greet(peers)
    lanes = blk.shape[1]
    lanes_of(out, net.x, lanes)[...] = blk[...]
    n_all[net.y, net.z, net.c] = tails[...].astype(BF)
    half = lanes // 2
    cuts = {None: (0, lanes), 0: (0, half), 1: (half, half)}

    def part(at, h):
        first, width = cuts[h]
        return out.at[:, pl.ds(pl.multiple_of(at * lanes + first, half), width)]

    for _ in merge([
        gather_small(net, n_all, pl.ds(0, 16), pl.ds(0, half), 0.0, 0.2),
        gather_small_turned(net, n_all, pl.ds(0, 16), pl.ds(half, half), 0.0, 0.3),
        ring(net, "x", part, lambda at: None, 0.0, 4.0),
        products(ham, ham2, pi, hp, h2p, turned),
    ]):
        pass
    net.finish()


def back(blk, tails, ham, ham2, pi):
    lanes = blk.shape[1]
    rows, n = ham.shape
    vm = pl.BlockSpec(memory_space=pltpu.VMEM)
    return pl.pallas_call(
        back_kernel,
        out_shape=[
            jax.ShapeDtypeStruct((blk.shape[0], 4 * lanes), BF),
            jax.ShapeDtypeStruct((NY, NZ, 2, 16, lanes), BF),
            jax.ShapeDtypeStruct((rows, pi.shape[1]), F32),
            jax.ShapeDtypeStruct((rows, pi.shape[1]), F32),
        ],
        in_specs=[vm] * 5,
        out_specs=[vm] * 4,
        scratch_shapes=[
            pltpu.VMEM((rows, n), BF),
            pltpu.SemaphoreType.DMA((48,)),
            pltpu.SemaphoreType.DMA((48,)),
        ],
        compiler_params=pltpu.CompilerParams(collective_id=2, has_side_effects=True, vmem_limit_bytes=22 * 1024 * 1024),
        cost_estimate=pl.CostEstimate(flops=3 * 10**10, bytes_accessed=2**20, transcendentals=0),
        name="back",
    )(blk, tails, ham, ham2, pi)


def sums(lead, coef, aux, g_row, pall, x, pay, held):
    q = g_row.shape[1]
    coupled = aux.shape[1]
    modes = aux.shape[0] // (2 * held.shape[0])
    leads = q // coupled
    hot = [[jnp.where(lead[k] == l, 1.0, 0.0) for l in range(leads)] for k in range(modes)]
    level, width, re, im, occ = ([coef[i, k] for k in range(modes)] for i in range(5))

    def chunk(t, carry):
        rows = pl.ds(pl.multiple_of(32 * t, 32), 32)
        part = [aux[pl.ds(pl.multiple_of(32 * t * 2 * modes, 32) + i, 32, stride=2 * modes), :] for i in range(2 * modes)]
        pall[x, rows, :] = jnp.concatenate(part, axis=1).astype(BF)
        turned = []
        for k in range(modes):
            turned.append(-width[k] * part[2 * k] - level[k] * part[2 * k + 1])
            turned.append(level[k] * part[2 * k] - width[k] * part[2 * k + 1])

        def summed(values):
            out = []
            for p in range(2):
                for l in range(leads):
                    total = hot[0][l] * values[p]
                    for k in range(1, modes):
                        total = total + hot[k][l] * values[2 * k + p]
                    out.append(total)
            return jnp.concatenate(out, axis=1)

        l_sum = summed(part)
        held[rows, :] = l_sum.astype(BF)
        for i, a in enumerate((l_sum, summed(turned))):
            a = a.reshape(2, 2, 8, 2 * q).astype(BF)
            for c in range(2):
                pay[c, t // 4, pl.ds(2 * lax.rem(t, 4), 2), pl.ds(8 * i, 8), :] = a[:, c]
        return carry

    lax.fori_loop(0, held.shape[0] // 32, chunk, 0)
    n_re = dot(held[:, :q], g_row, 0, 0)
    n_im = -dot(held[:, q:], g_row, 0, 0)
    n = jnp.concatenate([n_re, n_im], axis=1).astype(BF)
    pay[0, :, :, 24:32, :] = n.reshape(NY, NZ, 8, 2 * q)
    lane = lax.broadcasted_iota(jnp.int32, (8, 2 * q), 1)
    scal = jnp.zeros((8, 2 * q), F32)
    for i, weights in enumerate((re, im, [re[k] * occ[k] for k in range(modes)], [im[k] * occ[k] for k in range(modes)])):
        for l in range(leads):
            scal = jnp.where(lane == i * leads + l, sum(weights[k] * hot[k][l] for k in range(modes)), scal)
    pay[1, :, :, 24:32, :] = jnp.broadcast_to(scal.astype(BF), (NY, NZ, 8, 2 * q))


def modes_kernel(lead, coef, aux, hp, h2p, src, u, g, hg, out):
    k = pl.program_id(0)
    coupled = aux.shape[1]
    rows, q = g.shape
    modes = aux.shape[0] // (2 * rows)
    level, width, wr, wi, occ = (coef[i, k] for i in range(5))
    first = pl.multiple_of(lead[k] * coupled, coupled)
    re, im = pl.ds(first, coupled), pl.ds(pl.multiple_of(q + first, coupled), coupled)
    lr, li = -width, level
    ar, ai = 3 + 2 * H2 * lr, 2 * H2 * li
    cr = 3 * lr + 2 * H2 * (lr * lr - li * li)
    ci = 3 * li + 4 * H2 * lr * li
    er, ei = 4 * H2 * li, -3 - 4 * H2 * lr
    size = 64

    def chunk(t, carry):
        at = pl.ds(pl.multiple_of(size * t, size), size)
        gk, hgk = occ * g[at, re].astype(F32), 2 * H2 * occ * hg[at, re]
        br, bi = src[at, re] - gk, src[at, im] - gk
        tr = ar * br - ai * bi + u[at, re] - hgk
        ti = ar * bi + ai * br + u[at, im] + hgk
        start = pl.multiple_of(size * t * 2 * modes, size) + 2 * k
        at_re = pl.ds(start, size, stride=2 * modes)
        at_im = pl.ds(start + 1, size, stride=2 * modes)
        pr, pim = aux[at_re, :], aux[at_im, :]
        hr, hi = hp[at, :coupled], hp[at, coupled:]
        out[at_re, :] = cr * pr - ci * pim + er * hr - ei * hi - 2 * H2 * h2p[at, :coupled] + wr * tr - wi * ti
        out[at_im, :] = cr * pim + ci * pr + er * hi + ei * hr - 2 * H2 * h2p[at, coupled:] + wr * ti + wi * tr
        return carry

    lax.fori_loop(0, rows // size, chunk, 0)


def advance_modes(lead, coef, aux, hp, h2p, src, u, g, hg):
    rows = hp.shape[0]
    coupled = aux.shape[1]
    modes = aux.shape[0] // (2 * rows)
    sm = pl.BlockSpec(memory_space=pltpu.SMEM)
    block = pl.BlockSpec((rows, 2 * coupled), lambda k: (0, k))

    def whole(a):
        return pl.BlockSpec(a.shape, lambda k: (0,) * a.ndim)

    return pl.pallas_call(
        modes_kernel,
        grid=(modes,),
        out_shape=jax.ShapeDtypeStruct(aux.shape, F32),
        in_specs=[sm, sm, whole(aux), block, block] + [whole(a) for a in (src, u, g, hg)],
        out_specs=whole(aux),
        compiler_params=pltpu.CompilerParams(vmem_limit_bytes=24 * 1024 * 1024),
        cost_estimate=pl.CostEstimate(flops=64 * aux.size, bytes_accessed=12 * 1024 * 1024, transcendentals=0),
        name="modes",
    )(lead, coef, aux, hp, h2p, src, u, g, hg)


def by_lead(x, gamma):
    leads, coupled = gamma.shape[:2]
    return jnp.concatenate(
        [dot(x[:, l * coupled : (l + 1) * coupled], gamma[l]) for l in range(leads)], axis=1
    )


def shards(density, auxiliary, hamiltonian, coupling, lead_index, mode_level, mode_width, residue, occupation, lead_gamma):
    rows, cols = density.shape[1:]
    n = hamiltonian.shape[1]
    leads, coupled = coupling.shape
    q = leads * coupled
    modes = auxiliary.shape[1]
    n_mode = lax.axis_size("mode")
    n_row = lax.axis_size("row")
    x_pos, m_pos = lax.axis_index("row"), lax.axis_index("mode")
    row_start, col_start = x_pos * rows, m_pos * cols
    flat = coupling.reshape(-1)

    e_row = (row_start + jnp.arange(rows, dtype=jnp.int32)[:, None] == flat[None, :]).astype(BF)
    e_col = (col_start + jnp.arange(cols, dtype=jnp.int32)[:, None] == flat[None, :]).astype(BF)
    rho_t = jnp.swapaxes(density, 1, 2).astype(BF).reshape(2 * cols, rows)
    ham_ct = jnp.swapaxes(lax.dynamic_slice_in_dim(hamiltonian, col_start, cols, 1), 0, 1)

    coef = jnp.stack([mode_level, mode_width, residue[:, 0], residue[:, 1], occupation])
    aux = auxiliary.reshape(-1, coupled)
    blk = jnp.concatenate([ham_ct, rho_t], axis=0).reshape(3, cols, rows)
    first, hrho_t, ham2_c, pi_all, panel, ham2_all, whole, tails, scal, grow_full, he_row_b, hg_row, he_col = front(
        lead_index, coef, aux, blk, hamiltonian, flat[None], lead_gamma
    )
    g_row = lax.dynamic_slice_in_dim(grow_full, row_start, rows, 0)
    ham_c = first[0]
    piece = rows // n_mode
    pi_all = pi_all.reshape(n, -1)
    panel = panel.reshape(2, n, rows)
    ham2_all = ham2_all.reshape(n, rows)
    whole = whole.reshape(n_mode, 2 * piece, 2 * q)
    l1_b = whole[:, :piece].reshape(rows, 2 * q)
    m1 = whole[:, piece : 2 * piece].reshape(rows, 2 * q).astype(F32)
    scal = scal[0]
    w_sum, v_sum = scal[: 2 * leads], scal[2 * leads : 4 * leads]

    src = dot(panel, grow_full, 1, 0)
    src = jnp.concatenate([src[0], src[1]], axis=1)
    w_q = jnp.repeat(w_sum, coupled)
    v_q = jnp.repeat(v_sum, coupled)
    s_re, s_im = src[:, :q], src[:, q:]
    g_row_f = g_row.astype(F32)
    drive = jnp.concatenate(
        [w_q[:q] * s_re - w_q[q:] * s_im - (v_q[:q] - v_q[q:]) * g_row_f, w_q[:q] * s_im + w_q[q:] * s_re - (v_q[:q] + v_q[q:]) * g_row_f], axis=1
    )
    x_row = (3.0 * l1_b.astype(F32) + 2 * H2 * (m1 + drive)).astype(BF)
    p1 = jnp.concatenate([dot(e_col, l1_b[:, p * q : (p + 1) * q], 1, 1) for p in range(2)], 0)
    xe = jnp.concatenate([dot(e_col, x_row[:, p * q : (p + 1) * q], 1, 1) for p in range(2)], 0)
    rhoh_t = jnp.swapaxes(dot(jnp.concatenate([ham_c, ham2_c], 0), panel, 1, 1), 0, 1)
    rhoh_t, rhoh2_t = (rhoh_t[:, i * cols : (i + 1) * cols].reshape(2 * cols, rows) for i in range(2))
    y = hrho_t - 2.0 * rhoh_t + 2.0 * jnp.concatenate([-p1[cols:], p1[:cols]], 0)
    z = dot(lax.dynamic_slice_in_dim(ham_c, row_start, rows, 1), l1_b)
    owner = col_start // rows
    own_l = lax.dynamic_slice_in_dim(l1_b, col_start - owner * rows, cols, 0)
    own_x = lax.dynamic_slice_in_dim(x_row, col_start - owner * rows, cols, 0)
    mask = (x_pos == owner).astype(BF)
    blk = jnp.concatenate([y.astype(BF), z.astype(BF), own_l * mask, own_x * mask], 0)
    second, n_all, h_pi, h2_pi = back(blk, tails, hamiltonian, ham2_all, pi_all)
    f_all = n_all[..., :8, :].reshape(rows, 2 * q).astype(F32)
    n_all = n_all[:, :, 0, 8:].reshape(q, 2 * q)
    third = second[2 * cols :].astype(F32)
    third = sum(third[:, i * rows : (i + 1) * rows] for i in range(n_row))
    z, l_c, x_c = third[:cols], third[cols : 2 * cols], third[2 * cols :]
    hy = dot(second[: 2 * cols], hamiltonian, 1, 1)
    b_re = x_c[:, :q] + 4 * H2 * z[:, q:]
    b_im = -x_c[:, q:] + 4 * H2 * z[:, :q]
    back_re = dot(b_re.astype(BF), e_row, 1, 1)
    back_im = dot(b_im.astype(BF), e_row, 1, 1)
    l_cb = l_c.astype(BF)
    c1_re, c1_im = dot(l_cb[:, :q], he_row_b, 1, 1), -dot(l_cb[:, q:], he_row_b, 1, 1)
    c2_re, c2_im = dot(he_col, l1_b[:, :q], 1, 1), dot(he_col, l1_b[:, q:], 1, 1)
    d_re, d_im = c1_re - c2_re, c1_im - c2_im
    comm = hrho_t - rhoh_t
    base = -2 * H2 * (hy + rhoh2_t) + xe
    out_re = 3.0 * comm[cols:] + base[:cols] + back_re + 2 * H2 * d_im
    out_im = -3.0 * comm[:cols] + base[cols:] + back_im - 2 * H2 * d_re
    density_rate = jnp.swapaxes(jnp.stack([out_re, out_im]), 1, 2)

    lg = jnp.concatenate([by_lead(l1_b[:, p * q : (p + 1) * q], lead_gamma) for p in range(2)], 1)
    u = 2 * H2 * (f_all + lg + dot(e_row, n_all))
    auxiliary_rate = advance_modes(lead_index, coef, aux, h_pi, h2_pi, src, u, g_row, hg_row).reshape(auxiliary.shape)
    return density_rate, auxiliary_rate


def solution(mesh):
    in_specs = (
        P(None, "row", "mode"),
        P("row", "mode", None, None),
        P("row", None),
        P(),
        P("mode"),
        P("mode"),
        P("mode"),
        P("mode", None),
        P("mode"),
        P(),
    )
    out_specs = (P(None, "row", "mode"), P("row", "mode", None, None))
    return jax.shard_map(shards, mesh=mesh, in_specs=in_specs, out_specs=out_specs, check_vma=False)
```
